32 devices in a mesh: seq: 8 (over z, x), tp: 4 (over y, core).
Axes of the slice: x: 2, y: 2, z: 4, core: 2. Of those that a mesh axis runs over, the one named last changes fastest.
Arguments:
- queries: bfloat16 [1536, 6144], P('seq', 'tp'), may hold values from -400 to 400
- key_vectors: bfloat16 [1536, 1024], P('seq', 'tp'), may hold values from -8 to 8
- value_vectors: bfloat16 [1536, 1024], P('seq', 'tp'), may hold values from -6 to 6
- positions: int32 [1536], P('seq'), may hold values from 0 to 1535, as said below
- residual: bfloat16 [1536, 6144], P('seq', 'tp'), may hold values from -200 to 200
- norm_gain: float32 [1, 6144], P(None, 'tp'), may hold values from 0.5 to 1.5
- out_weight: bfloat16 [6144, 6144], P('tp'), may hold values from -0.3125 to 0.3125
Outputs:
- quantized: bfloat16 [1536, 6144], P('seq')
- token_scale: float32 [1536], P('seq')
- new_residual: bfloat16 [1536, 6144], P('seq', 'tp')
The draws below stay inside these ranges and needn't reach their ends.
Inputs may be any that keep to these rules, and one draw needn't show every extreme that they name: The positions are a permutation of 0 to 1535. Cut into 16 runs of 96 consecutive positions, the rows of one index of seq hold run r in their first 96 rows and run 2 * 8 - 1 - r in their last ones, both in increasing order, with r differing between the indices of seq.
All inputs are finite; a program needn't handle non-finite values. Where the reference program divides by a largest or mean magnitude, that divisor is 1e-20 or more.
Results may differ from the reference program's by a relative error of at most 0.012.
Values may be sent and summed in bfloat16 or wider, within the bound.
A program may use at most 64 MiB of HBM per device.

```python
import math
import jax
import jax.numpy as jnp
from jax import lax

D = 6144
Q_HEADS = 48
KV_HEADS = 8
HEAD = 128
TOK_DEV = 192
TOKENS = 1536
N_SEQ = 8
N_TP = 4


def shared_keys(key):
    inner_key = jax.random.fold_in(key, 21)
    shape = (TOKENS, KV_HEADS * HEAD)
    base_draw = jax.random.truncated_normal(inner_key, -5.0, 5.0, shape, jnp.float32)
    return base_draw


def draw_key_vectors(key, part):
    base_draw = shared_keys(key)
    return base_draw.astype(jnp.bfloat16)


def draw_queries(key, part):
    shape = (TOKENS, Q_HEADS * HEAD)
    noise_key = jax.random.fold_in(key, 23)
    base_draw = 2.0 * jax.random.truncated_normal(noise_key, -5.0, 5.0, shape, jnp.float32)
    return base_draw.astype(jnp.bfloat16)


def draw_positions(key, part):
    run_order = jax.random.permutation(jax.random.fold_in(key, 11), N_SEQ).astype(jnp.int32)
    half_rows = TOK_DEV // 2
    lane_index = jnp.arange(half_rows, dtype=jnp.int32)
    first_run = run_order[:, None] * half_rows + lane_index[None, :]
    second = (2 * N_SEQ - 1 - run_order)[:, None] * half_rows + lane_index[None, :]
    return jnp.concatenate([first_run, second], axis=1).reshape(TOKENS).astype(jnp.int32)


def draw_residual(key, part):
    noise_key = jax.random.fold_in(key, 31)
    column_key = jax.random.fold_in(key, 32)
    row_key = jax.random.fold_in(key, 33)
    column_index = jnp.arange(D, dtype=jnp.float32)
    column_scale = 3.0 ** (column_index / D) * jnp.exp(jax.random.uniform(column_key, (D,), jnp.float32, 0.0, 1.2))
    noise = jax.random.truncated_normal(noise_key, -5.0, 5.0, (TOKENS, D), jnp.float32)
    row_scale = jnp.exp(jax.random.uniform(row_key, (TOKENS, 1), jnp.float32, 0.0, math.log(10.0)))
    return (0.2 * noise * row_scale * column_scale[None, :]).astype(jnp.bfloat16)


def steps_of(stream_key, extent, shards, low, largest):
    gain, own = 1.0, jax.random.fold_in(stream_key, 6)
    for position, shards_of in shards:
        draws = jnp.exp(jax.random.uniform(jax.random.fold_in(own, position), (shards_of,), jnp.float32, low / len(shards), largest / len(shards)))
        gain = gain * jnp.repeat(draws, extent[position] // shards_of).reshape([-1 if axis == position else 1 for axis in range(len(extent))])
    return gain


def centred(stream_key, extent, scale, reach, shards=(), kind=jnp.bfloat16):
    loudness = steps_of(stream_key, extent, shards, -0.22, 0.18) if shards else 1.0
    values = jax.random.normal(stream_key, extent, jnp.float32) * scale * loudness
    return jnp.minimum(jnp.maximum(values, -reach), reach).astype(kind)


def setup_inputs(seed: int = 0) -> dict:
    splits = jax.random.split(jax.random.key(seed), 8)
    return {
        "queries": draw_queries(jax.random.fold_in(splits[7], 71), 0),
        "key_vectors": draw_key_vectors(jax.random.fold_in(splits[7], 71), 0),
        "value_vectors": centred(splits[2], (TOKENS, KV_HEADS * HEAD), 1.0, 6.0, ((0, 8), (1, 4))),
        "positions": draw_positions(jax.random.fold_in(splits[7], 71), 0),
        "residual": draw_residual(jax.random.fold_in(splits[7], 71), 0),
        "norm_gain": jnp.clip(1.0 + 0.1 * jax.random.normal(splits[5], (1, D), jnp.float32), 0.5, 1.5),
        "out_weight": centred(splits[6], (Q_HEADS * HEAD, D), (Q_HEADS * HEAD // 16) ** -0.5, 0.3125, ((0, 4),)),
    }


def reference(queries, key_vectors, value_vectors, positions, residual, norm_gain, out_weight):
    token_count = queries.shape[0]
    group_size = Q_HEADS // KV_HEADS
    score_scale = 1.0 / math.sqrt(HEAD)
    query_heads = queries.reshape(token_count, Q_HEADS, HEAD).transpose(1, 0, 2)
    key_heads = key_vectors.reshape(token_count, KV_HEADS, HEAD).transpose(1, 0, 2)
    value_heads = value_vectors.reshape(token_count, KV_HEADS, HEAD).transpose(1, 0, 2)
    block_rows = TOK_DEV
    block_count = token_count // block_rows
    query_blocks = query_heads.reshape(Q_HEADS, block_count, block_rows, HEAD)
    pos_blocks = positions.reshape(block_count, block_rows)

    def one_head(head_index):
        key_rows = key_heads[head_index // group_size]
        value_rows = value_heads[head_index // group_size]

        def one_block(block_pair):
            query_block, block_pos = block_pair
            scores = jnp.dot(query_block, key_rows.T, preferred_element_type=jnp.float32) * score_scale
            visible = positions[None, :] <= block_pos[:, None]
            scores = jnp.where(visible, scores, -1e+30)
            row_max = lax.optimization_barrier(jnp.max(scores, axis=1, keepdims=True))
            raw_weights = jnp.where(visible, jnp.exp(scores - row_max), 0.0)
            weight_sum = lax.optimization_barrier(jnp.sum(raw_weights, axis=1, keepdims=True))
            mixed = jnp.dot(raw_weights.astype(jnp.bfloat16), value_rows, preferred_element_type=jnp.float32)
            return (mixed / weight_sum).astype(jnp.bfloat16)
        return lax.map(one_block, (query_blocks[head_index], pos_blocks))
    attended = lax.map(one_head, jnp.arange(Q_HEADS, dtype=jnp.int32))
    attended = attended.reshape(Q_HEADS, token_count, HEAD).transpose(1, 0, 2).reshape(token_count, Q_HEADS * HEAD)
    group_width = Q_HEADS * HEAD // N_TP
    summed = residual.astype(jnp.float32)
    for group_index in range(N_TP):
        lower = group_index * group_width
        partial_value = jnp.dot(attended[:, lower:lower + group_width], out_weight[lower:lower + group_width], preferred_element_type=jnp.float32)
        partial_value = lax.optimization_barrier(partial_value.astype(jnp.bfloat16))
        summed = summed + partial_value.astype(jnp.float32)
    new_residual = summed.astype(jnp.bfloat16)
    mean_square = lax.optimization_barrier(jnp.mean(summed * summed, axis=1, keepdims=True))
    normed = summed * lax.rsqrt(mean_square + 1e-05) * norm_gain
    token_scale = lax.optimization_barrier(jnp.max(jnp.abs(normed), axis=1)) + 1e-06
    quantized = (normed / token_scale[:, None]).astype(jnp.bfloat16)
    return (quantized, token_scale, new_residual)
```

```python
import functools
import math

import jax
import jax.numpy as jnp
from jax import lax
from jax.experimental import pallas as pl
from jax.experimental.pallas import tpu as pltpu
from jax.sharding import PartitionSpec as P

HEAD = 128
LOG2E = 1.4426950408889634
MASKED = -1e30
MESH = pl.DeviceIdType.MESH
F32 = jnp.float32
BF16 = jnp.bfloat16


def kernel(
    dims,
    pos_hbm, key_hbm, value_hbm, gain_hbm, query_hbm, residual_hbm, weight_hbm,
    total_all, stat, gain_all, order_ref,
    kv, pos_all, key_raw, value_raw, query_raw, residual_raw, query, residual, weight,
    attended, part, from_core, pair,
    load_sem, kv_send, kv_recv, forward_send, pos_send, pos_recv, gain_send, gain_recv,
    core_send, core_recv, y_send, y_recv, out_send, out_recv, stat_send, stat_recv,
):
    n_seq, n_tp, group, kv_count, half, tile = dims
    n_y = n_tp // 2
    me = lax.axis_index("seq")
    tp = lax.axis_index("tp")
    core = lax.rem(tp, 2)
    y = tp // 2
    core_peer = tp + 1 - 2 * core
    partner = me + 1 - 2 * lax.rem(me, 2)
    model = weight.shape[1]
    tiles = model // tile
    slice_width = model // n_tp
    tiles_slice = slice_width // tile
    own = half // 2
    keys = n_seq * half

    barrier = pltpu.get_barrier_semaphore()
    for step in range(1, n_seq):
        pl.semaphore_signal(
            barrier, inc=1, device_id=(lax.rem(me + step, n_seq), tp), device_id_type=MESH
        )
    for step in range(1, n_tp):
        pl.semaphore_signal(
            barrier, inc=1, device_id=(me, lax.rem(tp + step, n_tp)), device_id_type=MESH
        )

    loads = [
        pltpu.make_async_copy(source, target, load_sem.at[index])
        for index, (source, target) in enumerate(
            (
                (pos_hbm, pos_all.at[me]),
                (key_hbm, key_raw),
                (value_hbm, value_raw),
                (gain_hbm, gain_all.at[tp]),
                (query_hbm, query_raw),
                (residual_hbm, residual_raw),
                (weight_hbm, weight),
            )
        )
    ]
    for load in loads:
        load.start()
    loads[0].wait()
    own_pos = pos_all[me]
    first = own_pos[0:1, 0:1].astype(F32)
    second = own_pos[0:1, half : half + 1].astype(F32)
    keep = jnp.where(first < second, 1.0, 0.0)
    order_ref[...] = jnp.broadcast_to(keep, order_ref.shape)

    def split(ref):
        top = ref[:half, :].astype(F32)
        bottom = ref[half:, :].astype(F32)
        low = top * keep + bottom * (1.0 - keep)
        high = bottom * keep + top * (1.0 - keep)
        return low.astype(BF16), high.astype(BF16)

    for index, ref in enumerate((key_raw, value_raw)):
        loads[1 + index].wait()
        low, high = split(ref)
        kv[0, me, index] = low
        kv[1, me, index] = high
    loads[3].wait()
    pl.semaphore_wait(barrier, n_seq + n_tp - 2)

    line = n_seq // 2
    order = []
    for step in range(1, line // 2 + 1):
        order.append(step)
        if line - step != step:
            order.append(line - step)
    sent = []

    def remote(src, dst, send, recv, device):
        copy = pltpu.make_async_remote_copy(
            src_ref=src, dst_ref=dst, send_sem=send, recv_sem=recv,
            device_id=device, device_id_type=MESH,
        )
        copy.start()
        sent.append(copy)
        return copy

    def landed(dst, recv):
        pltpu.make_async_remote_copy(
            src_ref=dst, dst_ref=dst, send_sem=recv, recv_sem=recv,
            device_id=(partner, tp), device_id_type=MESH,
        ).wait_recv()

    def send_line(phase):
        for step in order:
            target = lax.rem(me + 2 * step, n_seq)
            remote(
                kv.at[phase, me], kv.at[phase, me], kv_send.at[phase, step],
                kv_recv.at[phase, me], (target, tp),
            )

    def send_partner(phase):
        remote(
            kv.at[phase, me], kv.at[phase, me], kv_send.at[phase, 0],
            kv_recv.at[phase, me], (partner, tp),
        )

    def forward(phase, step):
        source = lax.rem(me + 2 * step, n_seq)
        landed(kv.at[phase, source], kv_recv.at[phase, source])
        remote(
            kv.at[phase, source], kv.at[phase, source], forward_send.at[phase, step],
            kv_recv.at[phase, source], (partner, tp),
        )

    def arrivals(phase):
        for step in range(line):
            source = lax.rem(partner + 2 * step, n_seq)
            landed(kv.at[phase, source], kv_recv.at[phase, source])

    send_partner(0)
    send_line(0)
    for step in range(1, n_seq):
        remote(
            pos_all.at[me], pos_all.at[me], pos_send.at[step], pos_recv.at[me],
            (lax.rem(me + step, n_seq), tp),
        )
    for step in range(1, n_tp):
        remote(
            gain_all.at[tp], gain_all.at[tp], gain_send.at[step], gain_recv.at[tp],
            (me, lax.rem(tp + step, n_tp)),
        )
    loads[4].wait()
    loads[5].wait()
    query[0], query[1] = split(query_raw)
    residual[0], residual[1] = split(residual_raw)
    for step in order:
        forward(0, step)
    send_line(1)
    send_partner(1)
    for step in range(1, n_seq):
        source = lax.rem(me + step, n_seq)
        landed(pos_all.at[source], pos_recv.at[source])
    arrivals(0)

    lanes = lax.broadcasted_iota(jnp.int32, (1, keys), 1)
    rows = lax.broadcasted_iota(jnp.int32, (half, 1), 0).astype(F32)

    def bias(phase):
        pick = jnp.minimum if phase == 0 else jnp.maximum

        def base(index):
            value = pos_all[index]
            return pick(value[0:1, 0:1].astype(F32), value[0:1, half : half + 1].astype(F32))

        key_pos = jnp.zeros((1, keys), F32)
        for source in range(n_seq):
            inside = (lanes >= source * half) & (lanes < (source + 1) * half)
            key_pos = jnp.where(
                inside, base(source) + (lanes - source * half).astype(F32), key_pos
            )
        return jnp.where(key_pos <= base(me) + rows, 0.0, MASKED)

    stack = group if keys <= 1024 else 1

    def attend(phase):
        mask = bias(phase)
        for head in range(0, kv_count * group, stack):
            kv_head = head // group
            columns = slice(kv_head * HEAD, (kv_head + 1) * HEAD)
            block = jnp.concatenate(
                [
                    query[phase, :, (head + i) * HEAD : (head + i + 1) * HEAD]
                    for i in range(stack)
                ],
                axis=0,
            )
            scores = []
            for piece in range(phase + 1):
                key_rows = kv[piece, :, 0, :, columns].reshape(keys, HEAD)
                value = lax.dot_general(
                    block, key_rows, (((1,), (1,)), ((), ())), preferred_element_type=F32
                ).reshape(stack, half, keys)
                scores.append(value + mask[None] if piece == phase else value)
            peak = jnp.max(scores[0], axis=2, keepdims=True)
            for value in scores[1:]:
                peak = jnp.maximum(peak, jnp.max(value, axis=2, keepdims=True))
            mixed = jnp.zeros((stack * half, HEAD), F32)
            total = jnp.zeros((stack, half, 1), F32)
            for piece, value in enumerate(scores):
                weights = jnp.exp2((value - peak) * (LOG2E / math.sqrt(HEAD)))
                total += jnp.sum(weights, axis=2, keepdims=True)
                value_rows = kv[piece, :, 1, :, columns].reshape(keys, HEAD)
                mixed += jnp.dot(
                    weights.astype(BF16).reshape(stack * half, keys), value_rows,
                    preferred_element_type=F32,
                )
            mixed = (mixed.reshape(stack, half, HEAD) / total).astype(BF16)
            for i in range(stack):
                attended[phase, :, (head + i) * HEAD : (head + i + 1) * HEAD] = mixed[i]

    def reduce_tile(phase, index):
        landed(from_core.at[phase, index], core_recv.at[phase, index])
        both = part[phase, index, core].astype(F32) + from_core[phase, index].astype(F32)
        pair[phase, y, index] = both.astype(BF16)
        for step in range(1, n_y):
            target = lax.rem(y + step, n_y) * 2 + core
            remote(
                pair.at[phase, y, index], pair.at[phase, y, index],
                y_send.at[phase, index, step], y_recv.at[phase, y, index], (me, target),
            )

    def project(phase, between):
        for index in range(tiles):
            columns = slice(index * tile, (index + 1) * tile)
            product = jnp.dot(
                attended[phase], weight[:, columns], preferred_element_type=F32
            )
            inner = (index % tiles_slice) * tile
            mine = jnp.where(tp == index // tiles_slice, 1.0, 0.0)
            product += residual[phase, :, inner : inner + tile].astype(F32) * mine
            part[phase, index] = product.astype(BF16).reshape(2, own, tile)
            remote(
                part.at[phase, index, 1 - core], from_core.at[phase, index],
                core_send.at[phase, index], core_recv.at[phase, index], (me, core_peer),
            )
            if index >= 1:
                reduce_tile(phase, index - 1)
            if index < len(between):
                between[index]()
        reduce_tile(phase, tiles - 1)
        for task in between[tiles:]:
            task()

    def finish(phase):
        square = jnp.zeros((own, 1), F32)
        peak = jnp.zeros((own, 1), F32)
        for index in range(tiles):
            for step in range(1, n_y):
                source = lax.rem(y + step, n_y)
                landed(pair.at[phase, source, index], y_recv.at[phase, source, index])
            total = pair[phase, 0, index].astype(F32)
            for source in range(1, n_y):
                total += pair[phase, source, index].astype(F32)
            inner = (index % tiles_slice) * tile
            part_of = index // tiles_slice
            total_all[phase, part_of, core, :, inner : inner + tile] = total.astype(BF16)
            block = total_all.at[phase, part_of, core, :, inner : inner + tile]
            remote(
                block, block, out_send.at[phase, index], out_recv.at[phase, index],
                (me, core_peer),
            )
            square += jnp.sum(total * total, axis=1, keepdims=True)
            scaled = total * gain_all[part_of, :, inner : inner + tile]
            peak = jnp.maximum(peak, jnp.max(jnp.abs(scaled), axis=1, keepdims=True))
        inverse = lax.rsqrt(square / model + 1e-5)
        token = inverse * peak + 1e-6
        stat[phase, core, 0] = jnp.broadcast_to(token, (own, 128))
        stat[phase, core, 1] = jnp.broadcast_to(inverse / token, (own, 128))
        remote(
            stat.at[phase, core], stat.at[phase, core], stat_send.at[phase],
            stat_recv.at[phase], (me, core_peer),
        )

    attend(0)
    loads[6].wait()
    project(0, [functools.partial(forward, 1, step) for step in order])
    arrivals(1)
    attend(1)
    project(1, [])
    for step in range(1, n_tp):
        source = lax.rem(tp + step, n_tp)
        landed(gain_all.at[source], gain_recv.at[source])
    finish(0)
    finish(1)
    for phase in range(2):
        for index in range(tiles):
            inner = (index % tiles_slice) * tile
            landed(
                total_all.at[phase, index // tiles_slice, 1 - core, :, inner : inner + tile],
                out_recv.at[phase, index],
            )
        landed(stat.at[phase, 1 - core], stat_recv.at[phase])
    for copy in sent:
        copy.wait_send()


def assemble(
    dims, total_all, stat, gain_all, order_ref, quant_hbm, scale_ref, stream_hbm,
    quant, stream, sem,
):
    n_tp, own, slice_width = dims
    tp = lax.axis_index("tp")
    swap = (jnp.max(order_ref[...]) < 0.5).astype(jnp.int32)
    copies = []

    def send(src, dst):
        copy = pltpu.make_async_copy(src, dst, sem.at[len(copies)])
        copy.start()
        copies.append(copy)

    scales = []
    for top in range(2):
        phase = swap if top == 0 else 1 - swap
        for core in range(2):
            rows = pl.ds((2 * top + core) * own, own)
            stream[top, core] = total_all[phase, tp, core]
            send(stream.at[top, core], stream_hbm.at[rows])
            scales.append(stat[phase, core, 0])
            factor = stat[phase, core, 1][:, 0:1]
            for part in range(n_tp):
                columns = slice(part * slice_width, (part + 1) * slice_width)
                value = total_all[phase, part, core].astype(F32) * gain_all[part]
                quant[top, core, :, columns] = (value * factor).astype(BF16)
            send(quant.at[top, core], quant_hbm.at[rows])
    scale = jnp.concatenate(scales, axis=0)
    count = 4 * own
    row = lax.broadcasted_iota(jnp.int32, (count, 128), 0)
    lane = lax.broadcasted_iota(jnp.int32, (count, 128), 1)
    pieces = [
        jnp.sum(jnp.where(row == lane + start, scale, 0.0), axis=0, keepdims=True)
        for start in range(0, count, 128)
    ]
    for index, piece in enumerate(pieces):
        width = min(128, count - 128 * index)
        scale_ref[:, 128 * index : 128 * index + width] = piece[:, :width]
    for copy in copies:
        copy.wait()


def on_device(n_seq, n_tp, queries, key_vectors, value_vectors, positions, residual, norm_gain, out_weight):
    token_rows, query_width = queries.shape
    half = token_rows // 2
    own = half // 2
    kv_width = key_vectors.shape[1]
    kv_count = kv_width // HEAD
    group = query_width // kv_width
    model = out_weight.shape[1]
    slice_width = residual.shape[1]
    tile = math.gcd(slice_width, 768)
    tiles = model // tile
    n_y = n_tp // 2
    vmem = pl.BlockSpec(memory_space=pltpu.VMEM)
    anywhere = pl.BlockSpec(memory_space=pl.ANY)
    dma = pltpu.SemaphoreType.DMA
    line = n_seq // 2
    middle = pl.pallas_call(
        functools.partial(kernel, (n_seq, n_tp, group, kv_count, half, tile)),
        out_shape=(
            pltpu.VMEM((2, n_tp, 2, own, slice_width), BF16),
            pltpu.VMEM((2, 2, 2, own, 128), F32),
            pltpu.VMEM((n_tp, 1, slice_width), F32),
            pltpu.VMEM((8, 128), F32),
        ),
        in_specs=[anywhere] * 7,
        out_specs=(vmem,) * 4,
        scratch_shapes=[
            pltpu.VMEM((2, n_seq, 2, half, kv_width), BF16),
            pltpu.VMEM((n_seq, 1, token_rows), jnp.int32),
            pltpu.VMEM(key_vectors.shape, BF16),
            pltpu.VMEM(value_vectors.shape, BF16),
            pltpu.VMEM(queries.shape, BF16),
            pltpu.VMEM(residual.shape, BF16),
            pltpu.VMEM((2, half, query_width), BF16),
            pltpu.VMEM((2, half, slice_width), BF16),
            pltpu.VMEM(out_weight.shape, BF16),
            pltpu.VMEM((2, half, query_width), BF16),
            pltpu.VMEM((2, tiles, 2, own, tile), BF16),
            pltpu.VMEM((2, tiles, own, tile), BF16),
            pltpu.VMEM((2, n_y, tiles, own, tile), BF16),
            dma((7,)),
            dma((2, line)),
            dma((2, n_seq)),
            dma((2, line)),
            dma((n_seq,)),
            dma((n_seq,)),
            dma((n_tp,)),
            dma((n_tp,)),
            dma((2, tiles)),
            dma((2, tiles)),
            dma((2, tiles, n_y)),
            dma((2, n_y, tiles)),
            dma((2, tiles)),
            dma((2, tiles)),
            dma((2,)),
            dma((2,)),
        ],
        compiler_params=pltpu.CompilerParams(
            collective_id=0, has_side_effects=True, vmem_limit_bytes=48 * 1024 * 1024
        ),
    )(
        *(
            pltpu.with_memory_space_constraint(value, pltpu.HBM)
            for value in (
                positions[None, :], key_vectors, value_vectors, norm_gain, queries, residual,
                out_weight,
            )
        )
    )
    quant, scale, stream = pl.pallas_call(
        functools.partial(assemble, (n_tp, own, slice_width)),
        out_shape=(
            jax.ShapeDtypeStruct((token_rows, model), BF16),
            jax.ShapeDtypeStruct((1, token_rows), F32),
            jax.ShapeDtypeStruct((token_rows, slice_width), BF16),
        ),
        in_specs=[vmem] * 4,
        out_specs=(anywhere, vmem, anywhere),
        scratch_shapes=[
            pltpu.VMEM((2, 2, own, model), BF16),
            pltpu.VMEM((2, 2, own, slice_width), BF16),
            dma((8,)),
        ],
        compiler_params=pltpu.CompilerParams(vmem_limit_bytes=12 * 1024 * 1024),
    )(*middle)
    return (quant, scale.reshape(token_rows), stream)


def solution(mesh):
    return jax.shard_map(
        functools.partial(on_device, mesh.shape["seq"], mesh.shape["tp"]),
        mesh=mesh,
        in_specs=(
            P("seq", "tp"),
            P("seq", "tp"),
            P("seq", "tp"),
            P("seq"),
            P("seq", "tp"),
            P(None, "tp"),
            P("tp", None),
        ),
        out_specs=(P("seq", None), P("seq"), P("seq", "tp")),
        check_vma=False,
    )
```

```python
import functools
import math

import jax
import jax.numpy as jnp
from jax import lax
from jax.experimental import pallas as pl
from jax.experimental.pallas import tpu as pltpu
from jax.sharding import PartitionSpec as P

HEAD = 128
LOG2E = 1.4426950408889634
MASKED = -1e30
MESH = pl.DeviceIdType.MESH
F32 = jnp.float32
BF16 = jnp.bfloat16


def kernel(
    dims,
    pos_hbm, key_hbm, value_hbm, gain_hbm, query_hbm, residual_hbm, weight_hbm,
    total_all, low_quant, stat, gain_all, order_ref,
    kv, pos_all, key_raw, value_raw, query_raw, residual_raw, query, residual, weight,
    attended, part, from_core, pair,
    load_sem, x_send, x_recv, z_send, z_recv, pos_send, pos_recv, gain_send, gain_recv,
    core_send, core_recv, y_send, y_recv, out_send, out_recv, stat_send, stat_recv,
):
    n_seq, n_tp, group, kv_count, half, tile = dims
    n_y = n_tp // 2
    me = lax.axis_index("seq")
    tp = lax.axis_index("tp")
    core = lax.rem(tp, 2)
    y = tp // 2
    core_peer = tp + 1 - 2 * core
    partner = me + 1 - 2 * lax.rem(me, 2)
    model = weight.shape[1]
    tiles = model // tile
    slice_width = model // n_tp
    tiles_slice = slice_width // tile
    own = half // 2
    keys = n_seq * half

    barrier = pltpu.get_barrier_semaphore()
    for step in range(1, n_seq):
        pl.semaphore_signal(
            barrier, inc=1, device_id=(lax.rem(me + step, n_seq), tp), device_id_type=MESH
        )
    for step in range(1, n_tp):
        pl.semaphore_signal(
            barrier, inc=1, device_id=(me, lax.rem(tp + step, n_tp)), device_id_type=MESH
        )

    loads = [
        pltpu.make_async_copy(source, target, load_sem.at[index])
        for index, (source, target) in enumerate(
            (
                (pos_hbm, pos_all.at[me]),
                (key_hbm, key_raw),
                (value_hbm, value_raw),
                (gain_hbm, gain_all.at[tp]),
                (query_hbm, query_raw),
                (residual_hbm, residual_raw),
                (weight_hbm, weight),
            )
        )
    ]
    for load in loads:
        load.start()
    loads[0].wait()
    own_pos = pos_all[me]
    first = own_pos[0:1, 0:1].astype(F32)
    second = own_pos[0:1, half : half + 1].astype(F32)
    keep = jnp.where(first < second, 1.0, 0.0)
    order_ref[...] = jnp.broadcast_to(keep, order_ref.shape)

    def split(ref):
        top = ref[:half, :].astype(F32)
        bottom = ref[half:, :].astype(F32)
        low = top * keep + bottom * (1.0 - keep)
        high = bottom * keep + top * (1.0 - keep)
        return low.astype(BF16), high.astype(BF16)

    for index, ref in enumerate((key_raw, value_raw)):
        loads[1 + index].wait()
        low, high = split(ref)
        for head in range(kv_count):
            columns = slice(head * HEAD, (head + 1) * HEAD)
            kv[0, me, head, index] = low[:, columns]
            kv[1, me, head, index] = high[:, columns]
    loads[3].wait()
    pl.semaphore_wait(barrier, n_seq + n_tp - 2)

    line = n_seq // 2
    row = me // 2
    column = lax.rem(me, 2)

    def remote(src, dst, send, recv, device, when=None):
        copy = pltpu.make_async_remote_copy(
            src_ref=src, dst_ref=dst, send_sem=send, recv_sem=recv,
            device_id=device, device_id_type=MESH,
        )
        if when is None:
            copy.start()
        else:
            pl.when(when)(copy.start)

    def landed(dst, recv):
        pltpu.make_async_remote_copy(
            src_ref=dst, dst_ref=dst, send_sem=recv, recv_sem=recv,
            device_id=(partner, tp), device_id_type=MESH,
        ).wait_recv()

    def left(src, send):
        pltpu.make_async_remote_copy(
            src_ref=src, dst_ref=src, send_sem=send, recv_sem=send,
            device_id=(partner, tp), device_id_type=MESH,
        ).wait_send()

    def at_row(offset):
        return lax.rem(me + 2 * offset + n_seq, n_seq)

    def inside(offset):
        return (row + offset >= 0) & (row + offset < line)

    def along(phase, source, head, offset, when):
        remote(
            kv.at[phase, source, head], kv.at[phase, source, head],
            z_send.at[phase, head, 0 if offset > 0 else 1],
            z_recv.at[phase, source // 2, head], (at_row(offset), tp), when,
        )

    def across(phase, source, head, when=None):
        remote(
            kv.at[phase, source, head], kv.at[phase, source, head],
            x_send.at[phase, head], x_recv.at[phase, head], (partner, tp), when,
        )

    def send_own(phase):
        for head in range(kv_count):
            across(phase, me, head)
            for offset in (-1, 1, -3, 3):
                if abs(offset) < line:
                    along(phase, me, head, offset, inside(offset))

    def relay(phase, distance):
        for head in range(kv_count):
            for side in (-1, 1):
                source = at_row(side * distance)
                there = inside(side * distance)

                @pl.when(there)
                def _():
                    landed(kv.at[phase, source, head], z_recv.at[phase, source // 2, head])

                if distance != 2:
                    along(phase, source, head, -side, there & inside(-side))
                if distance > 1:
                    across(phase, source, head, there)
            if distance == 1:
                for side in (-1, 1):
                    across(phase, at_row(side), head, inside(side))

    distances = [d for d in (1, 3, 2) if d < line] + list(range(4, line))

    def arrivals(phase):
        for head in range(kv_count):
            landed(kv.at[phase, 0:line, head], x_recv.at[phase, head])

    def left_all(phase):
        for head in range(kv_count):
            left(kv.at[phase, 0:line, head], x_send.at[phase, head])
            for index in range(line):
                for slot, side in enumerate((1, -1)):
                    room = line - 1 - index if side > 0 else index
                    behind = line - 1 - room
                    count = 0 if room < 1 else 1 + (room >= 3) + behind - (behind >= 2)
                    if count:

                        @pl.when(row == index)
                        def _():
                            left(kv.at[phase, 0:count, head], z_send.at[phase, head, slot])

    send_own(0)
    for step in range(1, n_seq):
        remote(
            pos_all.at[me], pos_all.at[me], pos_send.at[0], pos_recv.at[0],
            (lax.rem(me + step, n_seq), tp),
        )
    for step in range(1, n_tp):
        remote(
            gain_all.at[tp], gain_all.at[tp], gain_send.at[0], gain_recv.at[0],
            (me, lax.rem(tp + step, n_tp)),
        )
    relay(0, distances[0])
    loads[4].wait()
    loads[5].wait()
    query[0], query[1] = split(query_raw)
    residual[0], residual[1] = split(residual_raw)
    for distance in distances[1:]:
        relay(0, distance)
    send_own(1)
    landed(pos_all.at[0 : n_seq - 1], pos_recv.at[0])

    lanes = lax.broadcasted_iota(jnp.int32, (1, keys), 1)
    rows = lax.broadcasted_iota(jnp.int32, (half, 1), 0).astype(F32)

    def bias(phase):
        pick = jnp.minimum if phase == 0 else jnp.maximum

        def base(index):
            value = pos_all[index]
            return pick(value[0:1, 0:1].astype(F32), value[0:1, half : half + 1].astype(F32))

        key_pos = jnp.zeros((1, keys), F32)
        for source in range(n_seq):
            span = (lanes >= source * half) & (lanes < (source + 1) * half)
            key_pos = jnp.where(
                span, base(source) + (lanes - source * half).astype(F32), key_pos
            )
        return jnp.where(key_pos <= base(me) + rows, 0.0, MASKED)

    stack = group if keys <= 1024 else 1

    def attend(phase):
        mask = bias(phase)
        for head in range(0, kv_count * group, stack):
            kv_head = head // group
            block = jnp.concatenate(
                [
                    query[phase, :, (head + i) * HEAD : (head + i + 1) * HEAD]
                    for i in range(stack)
                ],
                axis=0,
            )
            scores = []
            for piece in range(phase + 1):
                key_rows = kv[piece, :, kv_head, 0].reshape(keys, HEAD)
                value = lax.dot_general(
                    block, key_rows, (((1,), (1,)), ((), ())), preferred_element_type=F32
                ).reshape(stack, half, keys)
                scores.append(value + mask[None] if piece == phase else value)
            peak = jnp.max(scores[0], axis=2, keepdims=True)
            for value in scores[1:]:
                peak = jnp.maximum(peak, jnp.max(value, axis=2, keepdims=True))
            mixed = jnp.zeros((stack * half, HEAD), F32)
            total = jnp.zeros((stack, half, 1), F32)
            for piece, value in enumerate(scores):
                weights = jnp.exp2((value - peak) * (LOG2E / math.sqrt(HEAD)))
                total += jnp.sum(weights, axis=2, keepdims=True)
                value_rows = kv[piece, :, kv_head, 1].reshape(keys, HEAD)
                mixed += jnp.dot(
                    weights.astype(BF16).reshape(stack * half, keys), value_rows,
                    preferred_element_type=F32,
                )
            mixed = (mixed.reshape(stack, half, HEAD) / total).astype(BF16)
            for i in range(stack):
                attended[phase, :, (head + i) * HEAD : (head + i + 1) * HEAD] = mixed[i]

    def reduce_tile(phase, index):
        landed(from_core.at[phase, index], core_recv.at[phase, index])
        both = part[phase, index, core].astype(F32) + from_core[phase, index].astype(F32)
        pair[phase, y, index] = both.astype(BF16)
        for step in range(1, n_y):
            target = lax.rem(y + step, n_y) * 2 + core
            remote(
                pair.at[phase, y, index], pair.at[phase, y, index],
                y_send.at[phase, step - 1], y_recv.at[phase, n_y - 1 - step, index], (me, target),
            )

    lag = min(2, tiles)

    def project(phase, between):
        for index in range(tiles):
            columns = slice(index * tile, (index + 1) * tile)
            product = jnp.dot(
                attended[phase], weight[:, columns], preferred_element_type=F32
            )
            inner = (index % tiles_slice) * tile
            mine = jnp.where(tp == index // tiles_slice, 1.0, 0.0)
            product += residual[phase, :, inner : inner + tile].astype(F32) * mine
            part[phase, index] = product.astype(BF16).reshape(2, own, tile)
            remote(
                part.at[phase, index, 1 - core], from_core.at[phase, index],
                core_send.at[phase], core_recv.at[phase, index], (me, core_peer),
            )
            if index >= lag:
                reduce_tile(phase, index - lag)
            for place, task in between:
                if min(place, tiles - 1) == index:
                    task()
        for index in range(tiles - lag, tiles):
            reduce_tile(phase, index)

    def finish(phase):
        square = jnp.zeros((own, 1), F32)
        peak = jnp.zeros((own, 1), F32)
        for index in range(tiles):
            for step in range(1, n_y):
                source = lax.rem(y + step, n_y)
                landed(pair.at[phase, source, index], y_recv.at[phase, step - 1, index])
            total = pair[phase, 0, index].astype(F32)
            for source in range(1, n_y):
                total += pair[phase, source, index].astype(F32)
            inner = (index % tiles_slice) * tile
            part_of = index // tiles_slice
            total_all[phase, part_of, core, :, inner : inner + tile] = total.astype(BF16)
            block = total_all.at[phase, part_of, core, :, inner : inner + tile]
            remote(
                block, block, out_send.at[phase], out_recv.at[phase],
                (me, core_peer),
            )
            square += jnp.sum(total * total, axis=1, keepdims=True)
            scaled = total * gain_all[part_of, :, inner : inner + tile]
            peak = jnp.maximum(peak, jnp.max(jnp.abs(scaled), axis=1, keepdims=True))
        inverse = lax.rsqrt(square / model + 1e-5)
        token = inverse * peak + 1e-6
        stat[phase, core, 0] = jnp.broadcast_to(token, (own, 128))
        stat[phase, core, 1] = jnp.broadcast_to(inverse / token, (own, 128))
        remote(
            stat.at[phase, core], stat.at[phase, core], stat_send.at[phase],
            stat_recv.at[phase], (me, core_peer),
        )

    def sends_left(phase):
        left_all(phase)
        left(part.at[phase, :, 1 - core], core_send.at[phase])
        for step in range(1, n_y):
            left(pair.at[phase, y], y_send.at[phase, step - 1])
        left(total_all.at[phase, :, core], out_send.at[phase])
        left(stat.at[phase, core], stat_send.at[phase])

    def totals_landed(phase):
        landed(total_all.at[phase, :, 1 - core], out_recv.at[phase])
        landed(stat.at[phase, 1 - core], stat_recv.at[phase])

    def normalize(phase):
        for part_of in range(n_tp):
            for owner in range(2):
                value = total_all[phase, part_of, owner].astype(F32) * gain_all[part_of]
                factor = stat[phase, owner, 1][:, 0:1]
                columns = slice(part_of * slice_width, (part_of + 1) * slice_width)
                low_quant[owner, :, columns] = (value * factor).astype(BF16)

    arrivals(0)
    attend(0)
    loads[6].wait()
    project(
        0, [(1 + 2 * i, functools.partial(relay, 1, d)) for i, d in enumerate(distances)]
    )
    arrivals(1)
    attend(1)
    project(1, [])
    landed(gain_all.at[0 : n_tp - 1], gain_recv.at[0])
    finish(0)
    totals_landed(0)
    normalize(0)
    sends_left(0)
    left(pos_all.at[0 : n_seq - 1], pos_send.at[0])
    left(gain_all.at[0 : n_tp - 1], gain_send.at[0])
    finish(1)
    totals_landed(1)
    sends_left(1)


def assemble(
    dims, total_all, low_quant, stat, gain_all, order_ref, quant_hbm, scale_hbm, stream_hbm,
    quant, scale_row, sem,
):
    n_tp, own, slice_width = dims
    tp = lax.axis_index("tp")
    swap = (jnp.max(order_ref[...]) < 0.5).astype(jnp.int32)
    copies = []

    def send(src, dst):
        copy = pltpu.make_async_copy(src, dst, sem.at[len(copies)])
        copy.start()
        copies.append(copy)

    def rows(phase, core):
        place = swap if phase == 0 else 1 - swap
        return pl.ds(pl.multiple_of((2 * place + core) * own, own), own)

    for core in range(2):
        send(low_quant.at[core], quant_hbm.at[rows(0, core)])
        for phase in range(2):
            send(total_all.at[phase, tp, core], stream_hbm.at[rows(phase, core)])
    for core in range(2):
        factor = stat[1, core, 1][:, 0:1]
        for part in range(n_tp):
            columns = slice(part * slice_width, (part + 1) * slice_width)
            value = total_all[1, part, core].astype(F32) * gain_all[part]
            quant[core, :, columns] = (value * factor).astype(BF16)
            send(quant.at[core, :, columns], quant_hbm.at[rows(1, core), columns])
    scale = jnp.concatenate(
        [stat[swap if top == 0 else 1 - swap, core, 0] for top in range(2) for core in range(2)],
        axis=0,
    )
    count = 4 * own
    row = lax.broadcasted_iota(jnp.int32, (count, 128), 0)
    lane = lax.broadcasted_iota(jnp.int32, (count, 128), 1)
    for start in range(0, count, 128):
        piece = jnp.sum(jnp.where(row == lane + start, scale, 0.0), axis=0, keepdims=True)
        width = min(128, count - start)
        scale_row[:, start : start + width] = piece[:, :width]
    send(scale_row, scale_hbm)
    for copy in copies:
        copy.wait()


def on_device(n_seq, n_tp, queries, key_vectors, value_vectors, positions, residual, norm_gain, out_weight):
    token_rows, query_width = queries.shape
    half = token_rows // 2
    own = half // 2
    kv_width = key_vectors.shape[1]
    kv_count = kv_width // HEAD
    group = query_width // kv_width
    model = out_weight.shape[1]
    slice_width = residual.shape[1]
    tile = math.gcd(slice_width, 512)
    tiles = model // tile
    n_y = n_tp // 2
    vmem = pl.BlockSpec(memory_space=pltpu.VMEM)
    anywhere = pl.BlockSpec(memory_space=pl.ANY)
    dma = pltpu.SemaphoreType.DMA
    line = n_seq // 2
    middle = pl.pallas_call(
        functools.partial(kernel, (n_seq, n_tp, group, kv_count, half, tile)),
        out_shape=(
            pltpu.VMEM((2, n_tp, 2, own, slice_width), BF16),
            pltpu.VMEM((2, own, model), BF16),
            pltpu.VMEM((2, 2, 2, own, 128), F32),
            pltpu.VMEM((n_tp, 1, slice_width), F32),
            pltpu.VMEM((8, 128), F32),
        ),
        in_specs=[anywhere] * 7,
        out_specs=(vmem,) * 5,
        scratch_shapes=[
            pltpu.VMEM((2, n_seq, kv_count, 2, half, HEAD), BF16),
            pltpu.VMEM((n_seq, 1, token_rows), jnp.int32),
            pltpu.VMEM(key_vectors.shape, BF16),
            pltpu.VMEM(value_vectors.shape, BF16),
            pltpu.VMEM(queries.shape, BF16),
            pltpu.VMEM(residual.shape, BF16),
            pltpu.VMEM((2, half, query_width), BF16),
            pltpu.VMEM((2, half, slice_width), BF16),
            pltpu.VMEM(out_weight.shape, BF16),
            pltpu.VMEM((2, half, query_width), BF16),
            pltpu.VMEM((2, tiles, 2, own, tile), BF16),
            pltpu.VMEM((2, tiles, own, tile), BF16),
            pltpu.VMEM((2, n_y, tiles, own, tile), BF16),
            dma((7,)),
            dma((2, kv_count)),
            dma((2, kv_count)),
            dma((2, kv_count, 2)),
            dma((2, line, kv_count)),
            dma((1,)),
            dma((1,)),
            dma((1,)),
            dma((1,)),
            dma((2,)),
            dma((2, tiles)),
            dma((2, n_y - 1)),
            dma((2, n_y - 1, tiles)),
            dma((2,)),
            dma((2,)),
            dma((2,)),
            dma((2,)),
        ],
        compiler_params=pltpu.CompilerParams(
            collective_id=0, has_side_effects=True, vmem_limit_bytes=48 * 1024 * 1024
        ),
    )(
        *(
            pltpu.with_memory_space_constraint(value, pltpu.HBM)
            for value in (
                positions[None, :], key_vectors, value_vectors, norm_gain, queries, residual,
                out_weight,
            )
        )
    )
    quant, scale, stream = pl.pallas_call(
        functools.partial(assemble, (n_tp, own, slice_width)),
        out_shape=(
            jax.ShapeDtypeStruct((token_rows, model), BF16),
            jax.ShapeDtypeStruct((1, token_rows), F32),
            jax.ShapeDtypeStruct((token_rows, slice_width), BF16),
        ),
        in_specs=[vmem] * 5,
        out_specs=(anywhere,) * 3,
        scratch_shapes=[
            pltpu.VMEM((2, own, model), BF16),
            pltpu.VMEM((1, token_rows), F32),
            dma((7 + 2 * n_tp,)),
        ],
        compiler_params=pltpu.CompilerParams(vmem_limit_bytes=12 * 1024 * 1024),
    )(*middle)
    return (quant, scale.reshape(token_rows), stream)


def solution(mesh):
    return jax.shard_map(
        functools.partial(on_device, mesh.shape["seq"], mesh.shape["tp"]),
        mesh=mesh,
        in_specs=(
            P("seq", "tp"),
            P("seq", "tp"),
            P("seq", "tp"),
            P("seq"),
            P("seq", "tp"),
            P(None, "tp"),
            P("tp", None),
        ),
        out_specs=(P("seq", None), P("seq"), P("seq", "tp")),
        check_vma=False,
    )
```

```python
import functools
import math

import jax
import jax.numpy as jnp
from jax import lax
from jax.experimental import pallas as pl
from jax.experimental.pallas import tpu as pltpu
from jax.sharding import PartitionSpec as P

HEAD = 128
LOG2E = 1.4426950408889634
MASKED = -1e30
MESH = pl.DeviceIdType.MESH
F32 = jnp.float32
BF16 = jnp.bfloat16


def kernel(
    dims,
    pos_hbm, key_hbm, value_hbm, gain_hbm, query_hbm, residual_hbm, weight_hbm,
    total_all, low_quant, stat, gain_all, order_ref,
    kv, pos_own, key_raw, value_raw, query_raw, residual_raw, query, residual, weight,
    attended, part, from_core, pair,
    load_sem, x_send, x_recv, z_send, z_recv, gain_send, gain_recv,
    core_send, core_recv, y_send, y_recv, out_send, out_recv, stat_send, stat_recv,
):
    n_seq, n_tp, group, kv_count, half, tiles = dims
    n_y = n_tp // 2
    me = lax.axis_index("seq")
    tp = lax.axis_index("tp")
    core = lax.rem(tp, 2)
    y = tp // 2
    core_peer = tp + 1 - 2 * core
    partner = me + 1 - 2 * lax.rem(me, 2)
    model = weight.shape[1]
    slice_width = model // n_tp
    own = half // 2
    keys = n_seq * half
    line = n_seq // 2
    row = me // 2
    column = lax.rem(me, 2)

    def at_row(offset):
        return lax.rem(me + 2 * offset + n_seq, n_seq)

    def inside(offset):
        return (row + offset >= 0) & (row + offset < line)

    barrier = pltpu.get_barrier_semaphore()
    pl.semaphore_signal(barrier, inc=1, device_id=(partner, tp), device_id_type=MESH)
    greetings = n_tp
    for offset in (1, -1, 3):
        if abs(offset) < line:

            @pl.when(inside(offset))
            def _():
                pl.semaphore_signal(
                    barrier, inc=1, device_id=(at_row(offset), tp), device_id_type=MESH
                )

            greetings += jnp.where(inside(-offset), 1, 0)
    for step in range(1, n_tp):
        pl.semaphore_signal(
            barrier, inc=1, device_id=(me, lax.rem(tp + step, n_tp)), device_id_type=MESH
        )

    loads = [
        pltpu.make_async_copy(source, target, load_sem.at[index])
        for index, (source, target) in enumerate(
            (
                (pos_hbm, pos_own),
                (key_hbm, key_raw),
                (value_hbm, value_raw),
                (gain_hbm, gain_all.at[tp]),
                (query_hbm, query_raw),
                (residual_hbm, residual_raw),
                (weight_hbm, weight),
            )
        )
    ]
    for load in loads:
        load.start()
    loads[0].wait()
    first = pos_own[0:1, 0:1]
    second = pos_own[0:1, half : half + 1]
    keep = jnp.where(first < second, 1.0, 0.0)
    tile_row = lax.broadcasted_iota(jnp.int32, (16, HEAD), 0)
    start = jnp.where(tile_row < 2, jnp.minimum(first, second), jnp.maximum(first, second))
    digit = jnp.where((tile_row & 1) == 0, start >> 6, start & 63)
    kv[0, row, column, 0, 2 * half :] = digit.astype(F32).astype(BF16)
    order_ref[...] = jnp.broadcast_to(keep, order_ref.shape)

    def split(ref):
        top = ref[:half, :].astype(F32)
        bottom = ref[half:, :].astype(F32)
        low = top * keep + bottom * (1.0 - keep)
        high = bottom * keep + top * (1.0 - keep)
        return low.astype(BF16), high.astype(BF16)

    for index, ref in enumerate((key_raw, value_raw)):
        loads[1 + index].wait()
        low, high = split(ref)
        for head in range(kv_count):
            columns = slice(head * HEAD, (head + 1) * HEAD)
            kind = slice(index * half, (index + 1) * half)
            kv[0, row, column, head, kind] = low[:, columns]
            kv[1, row, column, head, kind] = high[:, columns]
    loads[3].wait()
    pl.semaphore_wait(barrier, greetings)


    def remote(src, dst, send, recv, device, when=None):
        copy = pltpu.make_async_remote_copy(
            src_ref=src, dst_ref=dst, send_sem=send, recv_sem=recv,
            device_id=device, device_id_type=MESH,
        )
        if when is None:
            copy.start()
        else:
            pl.when(when)(copy.start)

    def landed(dst, recv):
        pltpu.make_async_remote_copy(
            src_ref=dst, dst_ref=dst, send_sem=recv, recv_sem=recv,
            device_id=(partner, tp), device_id_type=MESH,
        ).wait_recv()

    def left(src, send):
        pltpu.make_async_remote_copy(
            src_ref=src, dst_ref=src, send_sem=send, recv_sem=send,
            device_id=(partner, tp), device_id_type=MESH,
        ).wait_send()

    def span(phase, head):
        return slice(0, 2 * half + 16 * (phase == 0 and head == 0))

    def block(phase, source, head):
        return kv.at[phase, source // 2, lax.rem(source, 2), head, span(phase, head)]

    def along(phase, source, head, offset, when):
        side = 0 if offset > 0 else 1
        target = (at_row(offset), tp)
        remote(
            block(phase, source, head), block(phase, source, head),
            z_send.at[phase, head, side], z_recv.at[phase, source // 2, head], target, when,
        )

    def across(phase, source, head, when=None):
        remote(
            block(phase, source, head), block(phase, source, head),
            x_send.at[phase, head], x_recv.at[phase, head], (partner, tp), when,
        )

    def send_own(phase):
        for head in range(kv_count):
            across(phase, me, head)
            for offset in (-1, -3, 1) if phase == 0 else (-1, 1, -3, 3):
                if abs(offset) < line:
                    along(phase, me, head, offset, inside(offset))

    def relay(phase, side, distance):
        source = at_row(side * distance)
        there = inside(side * distance)
        for head in range(kv_count):

            @pl.when(there)
            def _():
                landed(block(phase, source, head), z_recv.at[phase, source // 2, head])

            if distance != 2 or (phase == 0 and side < 0):
                along(phase, source, head, -side, there & inside(-side))
            across(phase, source, head, there)

    relays = [(-1, d) for d in range(1, line)]
    relays += [(1, d) for d in (1, 3, 2) if d < line] + [(1, d) for d in range(4, line)]

    def arrivals(phase):
        for head in range(kv_count):
            landed(kv.at[phase, :, 0, head, span(phase, head)], x_recv.at[phase, head])

    def left_all(phase):
        for head in range(kv_count):
            left(kv.at[phase, :, 0, head, span(phase, head)], x_send.at[phase, head])
        for index in range(line):
            ahead = line - 1 - index
            counts = (
                1 + (phase == 1 and ahead >= 3) + index - (phase == 1 and index >= 2)
                if ahead
                else 0,
                1 + (index >= 3) + ahead - (ahead >= 2) if index else 0,
            )

            @pl.when(row == index)
            def _():
                for side, count in enumerate(counts):
                    if count == 0:
                        continue
                    for head in range(kv_count):
                        left(
                            kv.at[phase, 0:count, 0, head, span(phase, head)],
                            z_send.at[phase, head, side],
                        )

    send_own(0)
    for step in range(1, n_tp):
        remote(
            gain_all.at[tp], gain_all.at[tp], gain_send.at[0], gain_recv.at[0],
            (me, lax.rem(tp + step, n_tp)),
        )
    loads[4].wait()
    loads[5].wait()
    query[0], query[1] = split(query_raw)
    residual[0], residual[1] = split(residual_raw)
    for side, distance in relays:
        relay(0, side, distance)
    send_own(1)

    rows = lax.broadcasted_iota(jnp.int32, (half, 1), 0).astype(F32)

    def bias(phase, sources):
        lanes = lax.broadcasted_iota(jnp.int32, (1, len(sources) * half), 1)

        def base(index):
            digits = kv[0, index // 2, lax.rem(index, 2), 0, 2 * half :].astype(F32)
            return digits[2 * phase : 2 * phase + 1, 0:1] * 64.0 + digits[
                2 * phase + 1 : 2 * phase + 2, 0:1
            ]

        key_pos = jnp.zeros(lanes.shape, F32)
        for index, source in enumerate(sources):
            within = (lanes >= index * half) & (lanes < (index + 1) * half)
            key_pos = jnp.where(within, base(source) + (lanes - index * half).astype(F32), key_pos)
        return jnp.where(key_pos <= base(me) + rows, 0.0, MASKED)

    stack = group if keys <= 1024 else 1
    heads = range(0, kv_count * group, stack)
    slope = LOG2E / math.sqrt(HEAD)

    def queries_of(phase, head):
        return jnp.concatenate(
            [query[phase, :, (head + i) * HEAD : (head + i + 1) * HEAD] for i in range(stack)],
            axis=0,
        )

    def scores_of(block_rows, key_rows, mask):
        count = key_rows.shape[0]
        value = lax.dot_general(
            block_rows, key_rows, (((1,), (1,)), ((), ())), preferred_element_type=F32
        ).reshape(stack, half, count)
        return value if mask is None else value + mask[None]

    def weigh(value, peak, value_rows):
        weights = jnp.exp2((value - peak) * slope)
        mixed = jnp.dot(
            weights.astype(BF16).reshape(stack * half, value.shape[2]), value_rows,
            preferred_element_type=F32,
        ).reshape(stack, half, HEAD)
        return jnp.sum(weights, axis=2, keepdims=True), mixed

    def put(phase, head, mixed):
        for i in range(stack):
            attended[phase, :, (head + i) * HEAD : (head + i + 1) * HEAD] = mixed[i].astype(BF16)

    def attend_column(side, before):
        place = column if side == 0 else 1 - column
        mask = bias(0, [2 * index + place for index in range(line)])
        results = []
        for index, head in enumerate(heads):
            key_rows, value_rows = (
                kv[0, :, place, head // group, kind * half : (kind + 1) * half].reshape(
                    line * half, HEAD
                )
                for kind in range(2)
            )
            value = scores_of(queries_of(0, head), key_rows, mask)
            peak = jnp.max(value, axis=2, keepdims=True)
            if side == 0:
                results.append((peak, *weigh(value, peak, value_rows)))
                continue
            old_peak, old_total, old_mixed = before[index]
            peak = jnp.maximum(peak, old_peak)
            total, mixed = weigh(value, peak, value_rows)
            shrink = jnp.exp2((old_peak - peak) * slope)
            put(0, head, (mixed + old_mixed * shrink) / (total + old_total * shrink))
        return results

    def attend(phase):
        mask = bias(phase, list(range(n_seq)))
        for head in heads:
            kv_head = head // group
            block_rows = queries_of(phase, head)
            scores = [
                scores_of(
                    block_rows, kv[piece, :, :, kv_head, :half].reshape(keys, HEAD),
                    mask if piece == phase else None,
                )
                for piece in range(phase + 1)
            ]
            peak = jnp.max(scores[0], axis=2, keepdims=True)
            for value in scores[1:]:
                peak = jnp.maximum(peak, jnp.max(value, axis=2, keepdims=True))
            mixed = jnp.zeros((stack, half, HEAD), F32)
            total = jnp.zeros((stack, half, 1), F32)
            for piece, value in enumerate(scores):
                more, added = weigh(
                    value, peak, kv[piece, :, :, kv_head, half : 2 * half].reshape(keys, HEAD)
                )
                total += more
                mixed += added
            put(phase, head, mixed / total)

    def reduce_tile(phase, index):
        columns = tiles[index][2]
        landed(from_core.at[phase, :, columns], core_recv.at[phase, index])
        both = part[phase, core, :, columns].astype(F32) + from_core[phase, :, columns].astype(F32)
        pair[phase, y, :, columns] = both.astype(BF16)
        for step in range(1, n_y):
            target = lax.rem(y + step, n_y) * 2 + core
            remote(
                pair.at[phase, y, :, columns], pair.at[phase, y, :, columns],
                y_send.at[phase, step - 1], y_recv.at[phase, n_y - 1 - step, index], (me, target),
            )

    def project(phase, between):
        done = 0
        for index, (part_of, inner, columns) in enumerate(tiles):
            product = jnp.dot(
                attended[phase], weight[:, columns], preferred_element_type=F32
            )
            mine = jnp.where(tp == part_of, 1.0, 0.0)
            product += residual[phase, :, inner].astype(F32) * mine
            part[phase, 0, :, columns] = product[:own].astype(BF16)
            part[phase, 1, :, columns] = product[own:].astype(BF16)
            remote(
                part.at[phase, 1 - core, :, columns], from_core.at[phase, :, columns],
                core_send.at[phase], core_recv.at[phase, index], (me, core_peer),
            )
            ready = 1 if index < 4 else 2
            while done + ready <= index:
                reduce_tile(phase, done)
                done += 1
            for place, task in between:
                if min(place, len(tiles) - 1) == index:
                    task()
        for index in range(done, len(tiles)):
            reduce_tile(phase, index)

    def finish(phase):
        square = jnp.zeros((own, 1), F32)
        peak = jnp.zeros((own, 1), F32)
        for index, (part_of, inner, columns) in enumerate(tiles):
            for step in range(1, n_y):
                source = lax.rem(y + step, n_y)
                landed(pair.at[phase, source, :, columns], y_recv.at[phase, step - 1, index])
            total = pair[phase, 0, :, columns].astype(F32)
            for source in range(1, n_y):
                total += pair[phase, source, :, columns].astype(F32)
            total_all[phase, part_of, core, :, inner] = total.astype(BF16)
            piece = total_all.at[phase, part_of, core, :, inner]
            remote(piece, piece, out_send.at[phase], out_recv.at[phase], (me, core_peer))
            square += jnp.sum(total * total, axis=1, keepdims=True)
            scaled = total * gain_all[part_of, :, inner]
            peak = jnp.maximum(peak, jnp.max(jnp.abs(scaled), axis=1, keepdims=True))
        inverse = lax.rsqrt(square / model + 1e-5)
        token = inverse * peak + 1e-6
        stat[phase, core, 0] = jnp.broadcast_to(token, (own, 128))
        stat[phase, core, 1] = jnp.broadcast_to(inverse / token, (own, 128))
        remote(
            stat.at[phase, core], stat.at[phase, core], stat_send.at[phase],
            stat_recv.at[phase], (me, core_peer),
        )

    def sends_left(phase):
        left_all(phase)
        left(part.at[phase, 1 - core], core_send.at[phase])
        for step in range(1, n_y):
            left(pair.at[phase, y], y_send.at[phase, step - 1])
        left(total_all.at[phase, :, core], out_send.at[phase])
        left(stat.at[phase, core], stat_send.at[phase])

    def totals_landed(phase):
        landed(total_all.at[phase, :, 1 - core], out_recv.at[phase])
        landed(stat.at[phase, 1 - core], stat_recv.at[phase])

    def normalize(phase):
        for part_of in range(n_tp):
            for owner in range(2):
                value = total_all[phase, part_of, owner].astype(F32) * gain_all[part_of]
                factor = stat[phase, owner, 1][:, 0:1]
                columns = slice(part_of * slice_width, (part_of + 1) * slice_width)
                low_quant[owner, :, columns] = (value * factor).astype(BF16)

    near = attend_column(0, None)
    arrivals(0)
    attend_column(1, near)
    loads[6].wait()
    later = [d for d in (1, 3, 2) if d < line] + list(range(4, line))
    project(
        0,
        [
            (1 + 2 * i, functools.partial(relay, 1, side, distance))
            for i, distance in enumerate(later)
            for side in (-1, 1)
        ],
    )
    arrivals(1)
    attend(1)
    project(1, [])
    landed(gain_all.at[0 : n_tp - 1], gain_recv.at[0])
    finish(0)
    totals_landed(0)
    normalize(0)
    sends_left(0)
    left(gain_all.at[0 : n_tp - 1], gain_send.at[0])
    finish(1)
    totals_landed(1)
    sends_left(1)


def assemble(
    dims, total_all, low_quant, stat, gain_all, order_ref, quant_hbm, scale_hbm, stream_hbm,
    quant, scale_row, sem,
):
    n_tp, own, slice_width = dims
    tp = lax.axis_index("tp")
    swap = (jnp.max(order_ref[...]) < 0.5).astype(jnp.int32)

    def send(src, dst, index):
        pltpu.make_async_copy(src, dst, sem.at[index]).start()

    def rows(phase, core):
        place = swap if phase == 0 else 1 - swap
        return pl.ds(pl.multiple_of((2 * place + core) * own, own), own)

    for core in range(2):
        send(low_quant.at[core], quant_hbm.at[rows(0, core)], 0)
        for phase in range(2):
            send(total_all.at[phase, tp, core], stream_hbm.at[rows(phase, core)], 1)
    for core in range(2):
        factor = stat[1, core, 1][:, 0:1]
        for part in range(n_tp):
            columns = slice(part * slice_width, (part + 1) * slice_width)
            value = total_all[1, part, core].astype(F32) * gain_all[part]
            quant[core, :, columns] = (value * factor).astype(BF16)
            send(quant.at[core, :, columns], quant_hbm.at[rows(1, core), columns], 0)
    scale = jnp.concatenate(
        [stat[swap if top == 0 else 1 - swap, core, 0] for top in range(2) for core in range(2)],
        axis=0,
    )
    count = 4 * own
    row = lax.broadcasted_iota(jnp.int32, (count, 128), 0)
    lane = lax.broadcasted_iota(jnp.int32, (count, 128), 1)
    for start in range(0, count, 128):
        piece = jnp.sum(jnp.where(row == lane + start, scale, 0.0), axis=0, keepdims=True)
        width = min(128, count - start)
        scale_row[:, start : start + width] = piece[:, :width]
    send(scale_row, scale_hbm, 2)
    for index, array in enumerate((quant_hbm, stream_hbm, scale_hbm)):
        pltpu.make_async_copy(array, array, sem.at[index]).wait()


def tiles_of(n_tp, slice_width):
    if slice_width % 768:
        widths = [[slice_width]] * n_tp
    else:
        first = [256, 512] + [768] * (slice_width // 768 - 1)
        widths = [first] + [[768] * (slice_width // 768)] * (n_tp - 2) + [first[::-1]]
    tiles = []
    for index, row in enumerate(widths):
        inner = 0
        for width in row:
            start = index * slice_width + inner
            tiles.append((index, slice(inner, inner + width), slice(start, start + width)))
            inner += width
    return tiles


def on_device(n_seq, n_tp, queries, key_vectors, value_vectors, positions, residual, norm_gain, out_weight):
    token_rows, query_width = queries.shape
    half = token_rows // 2
    own = half // 2
    kv_width = key_vectors.shape[1]
    kv_count = kv_width // HEAD
    group = query_width // kv_width
    model = out_weight.shape[1]
    slice_width = residual.shape[1]
    tiles = tiles_of(n_tp, slice_width)
    count = len(tiles)
    n_y = n_tp // 2
    vmem = pl.BlockSpec(memory_space=pltpu.VMEM)
    anywhere = pl.BlockSpec(memory_space=pl.ANY)
    dma = pltpu.SemaphoreType.DMA
    line = n_seq // 2
    middle = pl.pallas_call(
        functools.partial(kernel, (n_seq, n_tp, group, kv_count, half, tiles)),
        out_shape=(
            pltpu.VMEM((2, n_tp, 2, own, slice_width), BF16),
            pltpu.VMEM((2, own, model), BF16),
            pltpu.VMEM((2, 2, 2, own, 128), F32),
            pltpu.VMEM((n_tp, 1, slice_width), F32),
            pltpu.VMEM((8, 128), F32),
        ),
        in_specs=[anywhere] * 7,
        out_specs=(vmem,) * 5,
        scratch_shapes=[
            pltpu.VMEM((2, line, 2, kv_count, 2 * half + 16, HEAD), BF16),
            pltpu.VMEM((1, token_rows), jnp.int32),
            pltpu.VMEM(key_vectors.shape, BF16),
            pltpu.VMEM(value_vectors.shape, BF16),
            pltpu.VMEM(queries.shape, BF16),
            pltpu.VMEM(residual.shape, BF16),
            pltpu.VMEM((2, half, query_width), BF16),
            pltpu.VMEM((2, half, slice_width), BF16),
            pltpu.VMEM(out_weight.shape, BF16),
            pltpu.VMEM((2, half, query_width), BF16),
            pltpu.VMEM((2, 2, own, model), BF16),
            pltpu.VMEM((2, own, model), BF16),
            pltpu.VMEM((2, n_y, own, model), BF16),
            dma((7,)),
            dma((2, kv_count)),
            dma((2, kv_count)),
            dma((2, kv_count, 2)),
            dma((2, line, kv_count)),
            dma((1,)),
            dma((1,)),
            dma((2,)),
            dma((2, count)),
            dma((2, n_y - 1)),
            dma((2, n_y - 1, count)),
            dma((2,)),
            dma((2,)),
            dma((2,)),
            dma((2,)),
        ],
        compiler_params=pltpu.CompilerParams(
            collective_id=0, has_side_effects=True, vmem_limit_bytes=48 * 1024 * 1024
        ),
    )(
        *(
            pltpu.with_memory_space_constraint(value, pltpu.HBM)
            for value in (
                positions[None, :], key_vectors, value_vectors, norm_gain, queries, residual,
                out_weight,
            )
        )
    )
    quant, scale, stream = pl.pallas_call(
        functools.partial(assemble, (n_tp, own, slice_width)),
        out_shape=(
            jax.ShapeDtypeStruct((token_rows, model), BF16),
            jax.ShapeDtypeStruct((1, token_rows), F32),
            jax.ShapeDtypeStruct((token_rows, slice_width), BF16),
        ),
        in_specs=[vmem] * 5,
        out_specs=(anywhere,) * 3,
        scratch_shapes=[
            pltpu.VMEM((2, own, model), BF16),
            pltpu.VMEM((1, token_rows), F32),
            dma((3,)),
        ],
        compiler_params=pltpu.CompilerParams(vmem_limit_bytes=12 * 1024 * 1024),
    )(*middle)
    return (quant, scale.reshape(token_rows), stream)


def solution(mesh):
    return jax.shard_map(
        functools.partial(on_device, mesh.shape["seq"], mesh.shape["tp"]),
        mesh=mesh,
        in_specs=(
            P("seq", "tp"),
            P("seq", "tp"),
            P("seq", "tp"),
            P("seq"),
            P("seq", "tp"),
            P(None, "tp"),
            P("tp", None),
        ),
        out_specs=(P("seq", None), P("seq"), P("seq", "tp")),
        check_vma=False,
    )
```

```python
import functools
import math

import jax
import jax.numpy as jnp
from jax import lax
from jax.experimental import pallas as pl
from jax.experimental.pallas import tpu as pltpu
from jax.sharding import PartitionSpec as P

HEAD = 128
LOG2E = 1.4426950408889634
MASKED = -1e30
MESH = pl.DeviceIdType.MESH
F32 = jnp.float32
BF16 = jnp.bfloat16


def kernel(
    dims,
    pos_hbm, key_hbm, value_hbm, gain_hbm, query_hbm, residual_hbm, weight_hbm,
    total_all, ready, stat, gain_all, order_ref,
    kv, pos_own, key_raw, value_raw, query_raw, residual_raw, query, residual, weight,
    attended, part, from_core, pair,
    load_sem, x_send, x_recv, z_send, z_recv, gain_send, gain_recv,
    core_send, core_recv, y_send, y_recv, out_send, out_recv, stat_send, stat_recv,
):
    n_seq, n_tp, group, kv_count, half, tiles = dims
    n_y = n_tp // 2
    me = lax.axis_index("seq")
    tp = lax.axis_index("tp")
    core = lax.rem(tp, 2)
    y = tp // 2
    core_peer = tp + 1 - 2 * core
    partner = me + 1 - 2 * lax.rem(me, 2)
    model = weight.shape[1]
    slice_width = model // n_tp
    own = half // 2
    keys = n_seq * half
    line = n_seq // 2
    row = me // 2
    column = lax.rem(me, 2)

    def at_row(offset):
        return lax.rem(me + 2 * offset + n_seq, n_seq)

    def inside(offset):
        return (row + offset >= 0) & (row + offset < line)

    loads = [
        pltpu.make_async_copy(source, target, load_sem.at[index])
        for index, (source, target) in enumerate(
            (
                (pos_hbm, pos_own),
                (key_hbm, key_raw),
                (value_hbm, value_raw),
                (gain_hbm, gain_all.at[tp]),
                (query_hbm, query_raw),
                (residual_hbm, residual_raw),
                (weight_hbm, weight),
            )
        )
    ]
    for load in loads[:3]:
        load.start()

    barrier = pltpu.get_barrier_semaphore()
    pl.semaphore_signal(barrier, inc=1, device_id=(partner, tp), device_id_type=MESH)
    greetings = n_tp
    for offset in (1, -1, 3):
        if abs(offset) < line:

            @pl.when(inside(offset))
            def _():
                pl.semaphore_signal(
                    barrier, inc=1, device_id=(at_row(offset), tp), device_id_type=MESH
                )

            greetings += jnp.where(inside(-offset), 1, 0)
    for step in range(1, n_tp):
        pl.semaphore_signal(
            barrier, inc=1, device_id=(me, lax.rem(tp + step, n_tp)), device_id_type=MESH
        )

    for load in loads[3:]:
        load.start()
    loads[0].wait()
    first = pos_own[0:1, 0:1]
    second = pos_own[0:1, half : half + 1]
    keep = jnp.where(first < second, 1.0, 0.0)
    tile_row = lax.broadcasted_iota(jnp.int32, (16, HEAD), 0)
    start = jnp.where(tile_row < 2, jnp.minimum(first, second), jnp.maximum(first, second))
    digit = jnp.where((tile_row & 1) == 0, start >> 6, start & 63)
    kv[0, row, column, 0, kv_count * half :] = digit.astype(F32).astype(BF16)
    order_ref[...] = jnp.broadcast_to(keep, order_ref.shape)

    def split(ref):
        top = ref[:half, :].astype(F32)
        bottom = ref[half:, :].astype(F32)
        low = top * keep + bottom * (1.0 - keep)
        high = bottom * keep + top * (1.0 - keep)
        return low.astype(BF16), high.astype(BF16)

    def place(kind, ref):
        loads[1 + kind].wait()
        for phase, rows in enumerate(split(ref)):
            for head in range(kv_count):
                kv[phase, row, column, kind, head * half : (head + 1) * half] = rows[
                    :, head * HEAD : (head + 1) * HEAD
                ]

    place(0, key_raw)
    pl.semaphore_wait(barrier, greetings)


    def remote(src, dst, send, recv, device, when=None):
        copy = pltpu.make_async_remote_copy(
            src_ref=src, dst_ref=dst, send_sem=send, recv_sem=recv,
            device_id=device, device_id_type=MESH,
        )
        if when is None:
            copy.start()
        else:
            pl.when(when)(copy.start)

    def landed(dst, recv):
        pltpu.make_async_remote_copy(
            src_ref=dst, dst_ref=dst, send_sem=recv, recv_sem=recv,
            device_id=(partner, tp), device_id_type=MESH,
        ).wait_recv()

    def left(src, send):
        pltpu.make_async_remote_copy(
            src_ref=src, dst_ref=src, send_sem=send, recv_sem=send,
            device_id=(partner, tp), device_id_type=MESH,
        ).wait_send()

    def span(phase, kind):
        return slice(0, kv_count * half + 16 * (phase == 0 and kind == 0))

    def block(phase, source, kind):
        return kv.at[phase, source // 2, lax.rem(source, 2), kind, span(phase, kind)]

    def along(phase, source, kind, offset, when):
        side = 0 if offset > 0 else 1
        target = (at_row(offset), tp)
        remote(
            block(phase, source, kind), block(phase, source, kind),
            z_send.at[phase, kind, side], z_recv.at[phase, source // 2, kind], target, when,
        )

    def across(phase, source, kind, when=None):
        remote(
            block(phase, source, kind), block(phase, source, kind),
            x_send.at[phase, kind], x_recv.at[phase, kind], (partner, tp), when,
        )

    def send_own(phase, kind):
        across(phase, me, kind)
        for offset in (-1, -3, 1) if phase == 0 else (-1, 1, -3, 3):
            if abs(offset) < line:
                along(phase, me, kind, offset, inside(offset))

    def relay(phase, side, distance):
        source = at_row(side * distance)
        there = inside(side * distance)
        for kind in range(2):

            @pl.when(there)
            def _():
                landed(block(phase, source, kind), z_recv.at[phase, source // 2, kind])

            if distance != 2 or (phase == 0 and side < 0):
                along(phase, source, kind, -side, there & inside(-side))
            across(phase, source, kind, there)

    relays = [(-1, d) for d in range(1, line)]
    relays += [(1, d) for d in (1, 3, 2) if d < line] + [(1, d) for d in range(4, line)]

    def arrivals(phase, kind):
        landed(kv.at[phase, :, 0, kind, span(phase, kind)], x_recv.at[phase, kind])

    def left_all(phase):
        for kind in range(2):
            left(kv.at[phase, :, 0, kind, span(phase, kind)], x_send.at[phase, kind])
        for index in range(line):
            akind = line - 1 - index
            counts = (
                1 + (phase == 1 and akind >= 3) + index - (phase == 1 and index >= 2)
                if akind
                else 0,
                1 + (index >= 3) + akind - (akind >= 2) if index else 0,
            )

            @pl.when(row == index)
            def _():
                for side, count in enumerate(counts):
                    if count == 0:
                        continue
                    for kind in range(2):
                        left(
                            kv.at[phase, 0:count, 0, kind, span(phase, kind)],
                            z_send.at[phase, kind, side],
                        )

    send_own(0, 0)
    place(1, value_raw)
    send_own(0, 1)
    loads[3].wait()
    for step in range(1, n_tp):
        remote(
            gain_all.at[tp], gain_all.at[tp], gain_send.at[0], gain_recv.at[0],
            (me, lax.rem(tp + step, n_tp)),
        )
    loads[4].wait()
    loads[5].wait()
    query[0], query[1] = split(query_raw)
    residual[0], residual[1] = split(residual_raw)
    for side, distance in relays:
        relay(0, side, distance)
    for kind in range(2):
        send_own(1, kind)

    rows = lax.broadcasted_iota(jnp.int32, (half, 1), 0).astype(F32)

    def bias(phase, sources):
        lanes = lax.broadcasted_iota(jnp.int32, (1, len(sources) * half), 1)

        def base(index):
            digits = kv[0, index // 2, lax.rem(index, 2), 0, kv_count * half :].astype(F32)
            return digits[2 * phase : 2 * phase + 1, 0:1] * 64.0 + digits[
                2 * phase + 1 : 2 * phase + 2, 0:1
            ]

        key_pos = jnp.zeros(lanes.shape, F32)
        for index, source in enumerate(sources):
            within = (lanes >= index * half) & (lanes < (index + 1) * half)
            key_pos = jnp.where(within, base(source) + (lanes - index * half).astype(F32), key_pos)
        return jnp.where(key_pos <= base(me) + rows, 0.0, MASKED)

    stack = group if keys <= 1024 else 1
    heads = range(0, kv_count * group, stack)
    slope = LOG2E / math.sqrt(HEAD)

    def queries_of(phase, head):
        return jnp.concatenate(
            [query[phase, :, (head + i) * HEAD : (head + i + 1) * HEAD] for i in range(stack)],
            axis=0,
        )

    def scores_of(block_rows, key_rows, mask):
        count = key_rows.shape[0]
        value = lax.dot_general(
            block_rows, key_rows, (((1,), (1,)), ((), ())), preferred_element_type=F32
        ).reshape(stack, half, count)
        return value if mask is None else value + mask[None]

    def weigh(value, peak):
        weights = jnp.exp2((value - peak) * slope)
        return jnp.sum(weights, axis=2, keepdims=True), weights.astype(BF16)

    def mix(weights, value_rows):
        return jnp.dot(
            weights.reshape(stack * half, weights.shape[2]), value_rows,
            preferred_element_type=F32,
        ).reshape(stack, half, HEAD)

    def head_rows(phase, place, kind, kv_head):
        span_of = slice(kv_head * half, (kv_head + 1) * half)
        if place is None:
            return kv[phase, :, :, kind, span_of].reshape(keys, HEAD)
        return kv[phase, :, place, kind, span_of].reshape(line * half, HEAD)

    def put(phase, head, mixed):
        for i in range(stack):
            attended[phase, :, (head + i) * HEAD : (head + i + 1) * HEAD] = mixed[i].astype(BF16)

    def column_scores(place):
        mask = bias(0, [2 * index + place for index in range(line)])
        values = []
        for head in heads:
            value = scores_of(
                queries_of(0, head), head_rows(0, place, 0, head // group), mask
            )
            values.append((value, jnp.max(value, axis=2, keepdims=True)))
        return values

    def attend_near():
        results = []
        for head, (value, peak) in zip(heads, column_scores(column)):
            total, weights = weigh(value, peak)
            results.append((peak, total, mix(weights, head_rows(0, column, 1, head // group))))
        return results

    def weigh_far(near):
        results = []
        for (old_peak, old_total, _), (value, peak) in zip(near, column_scores(1 - column)):
            peak = jnp.maximum(peak, old_peak)
            total, weights = weigh(value, peak)
            shrink = jnp.exp2((old_peak - peak) * slope)
            inverse = 1.0 / (total + old_total * shrink)
            results.append((weights, inverse, shrink * inverse))
        return results

    def attend_far(near, far):
        for head, (_, _, old_mixed), (weights, inverse, shrink) in zip(heads, near, far):
            mixed = mix(weights, head_rows(0, 1 - column, 1, head // group))
            put(0, head, mixed * inverse + old_mixed * shrink)

    def attend(phase):
        mask = bias(phase, list(range(n_seq)))
        for head in heads:
            kv_head = head // group
            block_rows = queries_of(phase, head)
            scores = [
                scores_of(
                    block_rows, head_rows(piece, None, 0, kv_head),
                    mask if piece == phase else None,
                )
                for piece in range(phase + 1)
            ]
            peak = jnp.max(scores[0], axis=2, keepdims=True)
            for value in scores[1:]:
                peak = jnp.maximum(peak, jnp.max(value, axis=2, keepdims=True))
            mixed = jnp.zeros((stack, half, HEAD), F32)
            total = jnp.zeros((stack, half, 1), F32)
            for piece, value in enumerate(scores):
                more, weights = weigh(value, peak)
                total += more
                mixed += mix(weights, head_rows(piece, None, 1, kv_head))
            put(phase, head, mixed / total)

    def reduce_tile(phase, index):
        columns = tiles[index][2]
        landed(from_core.at[phase, :, columns], core_recv.at[phase, index])
        both = part[phase, core, :, columns].astype(F32) + from_core[phase, :, columns].astype(F32)
        pair[phase, y, :, columns] = both.astype(BF16)
        for step in range(1, n_y):
            target = lax.rem(y + step, n_y) * 2 + core
            remote(
                pair.at[phase, y, :, columns], pair.at[phase, y, :, columns],
                y_send.at[phase, step - 1], y_recv.at[phase, n_y - 1 - step, index], (me, target),
            )

    def project(phase, between):
        done = 0
        for index, (part_of, inner, columns) in enumerate(tiles):
            product = jnp.dot(
                attended[phase], weight[:, columns], preferred_element_type=F32
            )
            mine = jnp.where(tp == part_of, 1.0, 0.0)
            product += residual[phase, :, inner].astype(F32) * mine
            part[phase, 0, :, columns] = product[:own].astype(BF16)
            part[phase, 1, :, columns] = product[own:].astype(BF16)
            remote(
                part.at[phase, 1 - core, :, columns], from_core.at[phase, :, columns],
                core_send.at[phase], core_recv.at[phase, index], (me, core_peer),
            )
            ready = 1 if index < 4 else 2
            while done + ready <= index:
                reduce_tile(phase, done)
                done += 1
            for place, task in between:
                if min(place, len(tiles) - 1) == index:
                    task()
        for index in range(done, len(tiles)):
            reduce_tile(phase, index)

    def finish(phase):
        square = jnp.zeros((own, 1), F32)
        peak = jnp.zeros((own, 1), F32)
        for index, (part_of, inner, columns) in enumerate(tiles):
            for step in range(1, n_y):
                source = lax.rem(y + step, n_y)
                landed(pair.at[phase, source, :, columns], y_recv.at[phase, step - 1, index])
            total = pair[phase, 0, :, columns].astype(F32)
            for source in range(1, n_y):
                total += pair[phase, source, :, columns].astype(F32)
            total_all[phase, part_of, core, :, inner] = total.astype(BF16)
            piece = total_all.at[phase, part_of, core, :, inner]
            remote(piece, piece, out_send.at[phase], out_recv.at[phase], (me, core_peer))
            square += jnp.sum(total * total, axis=1, keepdims=True)
            scaled = total * gain_all[part_of, :, inner]
            peak = jnp.maximum(peak, jnp.max(jnp.abs(scaled), axis=1, keepdims=True))
        inverse = lax.rsqrt(square / model + 1e-5)
        token = inverse * peak + 1e-6
        stat[phase, core, 0] = jnp.broadcast_to(token, (own, 128))
        stat[phase, core, 1] = jnp.broadcast_to(inverse / token, (own, 128))
        remote(
            stat.at[phase, core], stat.at[phase, core], stat_send.at[phase],
            stat_recv.at[phase], (me, core_peer),
        )

    def sends_left(phase):
        left_all(phase)
        left(part.at[phase, 1 - core], core_send.at[phase])
        for step in range(1, n_y):
            left(pair.at[phase, y], y_send.at[phase, step - 1])
        left(total_all.at[phase, :, core], out_send.at[phase])
        left(stat.at[phase, core], stat_send.at[phase])

    def totals_landed(phase):
        landed(total_all.at[phase, :, 1 - core], out_recv.at[phase])
        landed(stat.at[phase, 1 - core], stat_recv.at[phase])

    def normalize(phase, owner, slot):
        factor = stat[phase, owner, 1][:, 0:1]
        for part_of in range(n_tp):
            value = total_all[phase, part_of, owner].astype(F32) * gain_all[part_of]
            columns = slice(part_of * slice_width, (part_of + 1) * slice_width)
            ready[slot, :, columns] = (value * factor).astype(BF16)

    near = attend_near()
    arrivals(0, 0)
    far = weigh_far(near)
    arrivals(0, 1)
    attend_far(near, far)
    loads[6].wait()
    later = [d for d in (1, 3, 2) if d < line] + list(range(4, line))
    project(
        0,
        [
            (1 + 2 * i, functools.partial(relay, 1, side, distance))
            for i, distance in enumerate(later)
            for side in (-1, 1)
        ],
    )
    for kind in range(2):
        arrivals(1, kind)
    attend(1)
    project(1, [])
    landed(gain_all.at[0 : n_tp - 1], gain_recv.at[0])
    finish(0)
    totals_landed(0)
    for owner in range(2):
        normalize(0, owner, owner)
    sends_left(0)
    left(gain_all.at[0 : n_tp - 1], gain_send.at[0])
    finish(1)
    normalize(1, core, 2)
    totals_landed(1)
    sends_left(1)


def assemble(
    dims, total_all, ready, stat, gain_all, order_ref, quant_hbm, scale_hbm, stream_hbm,
    quant, scale_row, sem,
):
    n_tp, own, slice_width = dims
    tp = lax.axis_index("tp")
    swap = (order_ref[0, 0] < 0.5).astype(jnp.int32)
    mine = lax.rem(tp, 2)

    def send(src, dst, index):
        pltpu.make_async_copy(src, dst, sem.at[index]).start()

    def rows(phase, core):
        place = swap if phase == 0 else 1 - swap
        return pl.ds(pl.multiple_of((2 * place + core) * own, own), own)

    for core in range(2):
        send(ready.at[core], quant_hbm.at[rows(0, core)], 0)
    send(ready.at[2], quant_hbm.at[rows(1, mine)], 0)
    for core in range(2):
        for phase in range(2):
            send(total_all.at[phase, tp, core], stream_hbm.at[rows(phase, core)], 1)
    factor = stat[1, 1 - mine, 1][:, 0:1]
    for part in range(n_tp):
        columns = slice(part * slice_width, (part + 1) * slice_width)
        value = total_all[1, part, 1 - mine].astype(F32) * gain_all[part]
        quant[:, columns] = (value * factor).astype(BF16)
        send(quant.at[:, columns], quant_hbm.at[rows(1, 1 - mine), columns], 0)
    scale = jnp.concatenate(
        [stat[swap if top == 0 else 1 - swap, core, 0] for top in range(2) for core in range(2)],
        axis=0,
    )
    count = 4 * own
    row = lax.broadcasted_iota(jnp.int32, (count, 128), 0)
    lane = lax.broadcasted_iota(jnp.int32, (count, 128), 1)
    for start in range(0, count, 128):
        piece = jnp.sum(jnp.where(row == lane + start, scale, 0.0), axis=0, keepdims=True)
        width = min(128, count - start)
        scale_row[:, start : start + width] = piece[:, :width]
    send(scale_row, scale_hbm, 2)
    for index, array in enumerate((quant_hbm, stream_hbm, scale_hbm)):
        pltpu.make_async_copy(array, array, sem.at[index]).wait()


def tiles_of(n_tp, slice_width):
    if slice_width % 768:
        widths = [[slice_width]] * n_tp
    else:
        first = [256, 512] + [768] * (slice_width // 768 - 1)
        widths = [first] + [[768] * (slice_width // 768)] * (n_tp - 2) + [first[::-1]]
    tiles = []
    for index, row in enumerate(widths):
        inner = 0
        for width in row:
            start = index * slice_width + inner
            tiles.append((index, slice(inner, inner + width), slice(start, start + width)))
            inner += width
    return tiles


def on_device(n_seq, n_tp, queries, key_vectors, value_vectors, positions, residual, norm_gain, out_weight):
    token_rows, query_width = queries.shape
    half = token_rows // 2
    own = half // 2
    kv_width = key_vectors.shape[1]
    kv_count = kv_width // HEAD
    group = query_width // kv_width
    model = out_weight.shape[1]
    slice_width = residual.shape[1]
    tiles = tiles_of(n_tp, slice_width)
    count = len(tiles)
    n_y = n_tp // 2
    vmem = pl.BlockSpec(memory_space=pltpu.VMEM)
    anywhere = pl.BlockSpec(memory_space=pl.ANY)
    dma = pltpu.SemaphoreType.DMA
    line = n_seq // 2
    middle = pl.pallas_call(
        functools.partial(kernel, (n_seq, n_tp, group, kv_count, half, tiles)),
        out_shape=(
            pltpu.VMEM((2, n_tp, 2, own, slice_width), BF16),
            pltpu.VMEM((3, own, model), BF16),
            pltpu.VMEM((2, 2, 2, own, 128), F32),
            pltpu.VMEM((n_tp, 1, slice_width), F32),
            pltpu.VMEM((8, 128), F32),
        ),
        in_specs=[anywhere] * 7,
        out_specs=(vmem,) * 5,
        scratch_shapes=[
            pltpu.VMEM((2, line, 2, 2, kv_count * half + 16, HEAD), BF16),
            pltpu.VMEM((1, token_rows), jnp.int32),
            pltpu.VMEM(key_vectors.shape, BF16),
            pltpu.VMEM(value_vectors.shape, BF16),
            pltpu.VMEM(queries.shape, BF16),
            pltpu.VMEM(residual.shape, BF16),
            pltpu.VMEM((2, half, query_width), BF16),
            pltpu.VMEM((2, half, slice_width), BF16),
            pltpu.VMEM(out_weight.shape, BF16),
            pltpu.VMEM((2, half, query_width), BF16),
            pltpu.VMEM((2, 2, own, model), BF16),
            pltpu.VMEM((2, own, model), BF16),
            pltpu.VMEM((2, n_y, own, model), BF16),
            dma((7,)),
            dma((2, 2)),
            dma((2, 2)),
            dma((2, 2, 2)),
            dma((2, line, 2)),
            dma((1,)),
            dma((1,)),
            dma((2,)),
            dma((2, count)),
            dma((2, n_y - 1)),
            dma((2, n_y - 1, count)),
            dma((2,)),
            dma((2,)),
            dma((2,)),
            dma((2,)),
        ],
        compiler_params=pltpu.CompilerParams(
            collective_id=0, has_side_effects=True, vmem_limit_bytes=48 * 1024 * 1024
        ),
    )(
        *(
            pltpu.with_memory_space_constraint(value, pltpu.HBM)
            for value in (
                positions[None, :], key_vectors, value_vectors, norm_gain, queries, residual,
                out_weight,
            )
        )
    )
    quant, scale, stream = pl.pallas_call(
        functools.partial(assemble, (n_tp, own, slice_width)),
        out_shape=(
            jax.ShapeDtypeStruct((token_rows, model), BF16),
            jax.ShapeDtypeStruct((1, token_rows), F32),
            jax.ShapeDtypeStruct((token_rows, slice_width), BF16),
        ),
        in_specs=[vmem] * 5,
        out_specs=(anywhere,) * 3,
        scratch_shapes=[
            pltpu.VMEM((own, model), BF16),
            pltpu.VMEM((1, token_rows), F32),
            dma((3,)),
        ],
        compiler_params=pltpu.CompilerParams(vmem_limit_bytes=12 * 1024 * 1024),
    )(*middle)
    return (quant, scale.reshape(token_rows), stream)


def solution(mesh):
    return jax.shard_map(
        functools.partial(on_device, mesh.shape["seq"], mesh.shape["tp"]),
        mesh=mesh,
        in_specs=(
            P("seq", "tp"),
            P("seq", "tp"),
            P("seq", "tp"),
            P("seq"),
            P("seq", "tp"),
            P(None, "tp"),
            P("tp", None),
        ),
        out_specs=(P("seq", None), P("seq"), P("seq", "tp")),
        check_vma=False,
    )
```

```python
import functools
import math

import jax
import jax.numpy as jnp
from jax import lax
from jax.experimental import pallas as pl
from jax.experimental.pallas import tpu as pltpu
from jax.sharding import PartitionSpec as P

HEAD = 128
LOG2E = 1.4426950408889634
MASKED = -1e30
MESH = pl.DeviceIdType.MESH
F32 = jnp.float32
BF16 = jnp.bfloat16


def kernel(
    dims,
    pos_hbm, key_hbm, value_hbm, gain_hbm, query_hbm, residual_hbm, weight_hbm,
    total_all, ready, stat, gain_all, order_ref,
    kv, pos_own, key_raw, value_raw, query_raw, residual_raw, query, residual, weight,
    attended, part, from_core, pair,
    load_sem, x_send, x_recv, z_send, z_recv, gain_send, gain_recv,
    core_send, core_recv, y_send, y_recv, out_send, out_recv, stat_send, stat_recv,
):
    n_seq, n_tp, group, kv_count, half, tiles = dims
    n_y = n_tp // 2
    me = lax.axis_index("seq")
    tp = lax.axis_index("tp")
    core = lax.rem(tp, 2)
    y = tp // 2
    core_peer = tp + 1 - 2 * core
    partner = me + 1 - 2 * lax.rem(me, 2)
    model = weight.shape[1]
    slice_width = model // n_tp
    own = half // 2
    keys = n_seq * half
    line = n_seq // 2
    row = me // 2
    column = lax.rem(me, 2)

    def at_row(offset):
        return lax.rem(me + 2 * offset + n_seq, n_seq)

    def inside(offset):
        return (row + offset >= 0) & (row + offset < line)

    loads = [
        pltpu.make_async_copy(source, target, load_sem.at[index])
        for index, (source, target) in enumerate(
            (
                (pos_hbm, pos_own),
                (key_hbm, key_raw),
                (value_hbm, value_raw),
                (gain_hbm, gain_all.at[tp]),
                (query_hbm, query_raw),
                (residual_hbm, residual_raw),
                (weight_hbm, weight),
            )
        )
    ]
    for load in loads[:3]:
        load.start()

    barrier = pltpu.get_barrier_semaphore()
    pl.semaphore_signal(barrier, inc=1, device_id=(partner, tp), device_id_type=MESH)
    greetings = n_tp
    for offset in (1, -1, 3):
        if abs(offset) < line:

            @pl.when(inside(offset))
            def _():
                pl.semaphore_signal(
                    barrier, inc=1, device_id=(at_row(offset), tp), device_id_type=MESH
                )

            greetings += jnp.where(inside(-offset), 1, 0)
    for step in range(1, n_tp):
        pl.semaphore_signal(
            barrier, inc=1, device_id=(me, lax.rem(tp + step, n_tp)), device_id_type=MESH
        )

    for load in loads[3:]:
        load.start()
    loads[0].wait()
    first = pos_own[0:1, 0:1]
    second = pos_own[0:1, half : half + 1]
    keep = jnp.where(first < second, 1.0, 0.0)
    tile_row = lax.broadcasted_iota(jnp.int32, (16, HEAD), 0)
    start = jnp.where(tile_row < 2, jnp.minimum(first, second), jnp.maximum(first, second))
    digit = jnp.where((tile_row & 1) == 0, start >> 6, start & 63)
    kv[0, row, column, 0, kv_count * half :] = digit.astype(F32).astype(BF16)
    order_ref[...] = jnp.broadcast_to(keep, order_ref.shape)

    def split(ref):
        top = ref[:half, :].astype(F32)
        bottom = ref[half:, :].astype(F32)
        low = top * keep + bottom * (1.0 - keep)
        high = bottom * keep + top * (1.0 - keep)
        return low.astype(BF16), high.astype(BF16)

    def place(kind, ref):
        loads[1 + kind].wait()
        for phase, rows in enumerate(split(ref)):
            for head in range(kv_count):
                kv[phase, row, column, kind, head * half : (head + 1) * half] = rows[
                    :, head * HEAD : (head + 1) * HEAD
                ]

    place(0, key_raw)
    pl.semaphore_wait(barrier, greetings)


    def remote(src, dst, send, recv, device, when=None):
        copy = pltpu.make_async_remote_copy(
            src_ref=src, dst_ref=dst, send_sem=send, recv_sem=recv,
            device_id=device, device_id_type=MESH,
        )
        if when is None:
            copy.start()
        else:
            pl.when(when)(copy.start)

    def landed(dst, recv):
        pltpu.make_async_remote_copy(
            src_ref=dst, dst_ref=dst, send_sem=recv, recv_sem=recv,
            device_id=(partner, tp), device_id_type=MESH,
        ).wait_recv()

    def left(src, send):
        pltpu.make_async_remote_copy(
            src_ref=src, dst_ref=src, send_sem=send, recv_sem=send,
            device_id=(partner, tp), device_id_type=MESH,
        ).wait_send()

    def pieces_of(rows, place, kind):
        if kind < 2:
            return kv.at[0, rows, place, kind, 0 : kv_count * half + 16 * (1 - kind)]
        return kv.at[1, rows, place, :, 0 : kv_count * half]

    def block(source, kind):
        return pieces_of(source // 2, lax.rem(source, 2), kind)

    def along(source, kind, offset, when):
        remote(
            block(source, kind), block(source, kind),
            z_send.at[kind, 0 if offset > 0 else 1], z_recv.at[kind, source // 2],
            (at_row(offset), tp), when,
        )

    def across(source, kind, when=None):
        remote(
            block(source, kind), block(source, kind), x_send.at[kind], x_recv.at[kind],
            (partner, tp), when,
        )

    def send_own(kind):
        across(me, kind)
        for offset in (-1, -3, 1) if kind < 2 else (-1, 1, -3, 3):
            if abs(offset) < line:
                along(me, kind, offset, inside(offset))

    def relay(kinds, side, distance):
        source = at_row(side * distance)
        there = inside(side * distance)
        for kind in kinds:

            @pl.when(there)
            def _():
                landed(block(source, kind), z_recv.at[kind, source // 2])

            if distance != 2 or (kind < 2 and side < 0):
                along(source, kind, -side, there & inside(-side))
            across(source, kind, there)

    relays = [(-1, d) for d in range(1, line)]
    relays += [(1, d) for d in (1, 3, 2) if d < line] + [(1, d) for d in range(4, line)]

    def arrivals(kind):
        landed(pieces_of(slice(0, line), 0, kind), x_recv.at[kind])

    def left_all():
        for kind in range(3):
            left(pieces_of(slice(0, line), 0, kind), x_send.at[kind])
        for index in range(line):
            ahead = line - 1 - index

            @pl.when(row == index)
            def _():
                for kind in range(3):
                    direct = kind == 2
                    counts = (
                        1 + (direct and ahead >= 3) + index - (direct and index >= 2)
                        if ahead
                        else 0,
                        1 + (index >= 3) + ahead - (ahead >= 2) if index else 0,
                    )
                    for side, count in enumerate(counts):
                        if count:
                            left(pieces_of(slice(0, count), 0, kind), z_send.at[kind, side])

    send_own(0)
    place(1, value_raw)
    send_own(1)
    loads[3].wait()
    for step in range(1, n_tp):
        remote(
            gain_all.at[tp], gain_all.at[tp], gain_send.at[0], gain_recv.at[0],
            (me, lax.rem(tp + step, n_tp)),
        )
    loads[4].wait()
    loads[5].wait()
    query[0], query[1] = split(query_raw)
    residual[0], residual[1] = split(residual_raw)
    for side, distance in relays:
        relay((0, 1), side, distance)
    send_own(2)

    rows = lax.broadcasted_iota(jnp.int32, (half, 1), 0).astype(F32)

    def bias(phase, sources):
        lanes = lax.broadcasted_iota(jnp.int32, (1, len(sources) * half), 1)

        def base(index):
            digits = kv[0, index // 2, lax.rem(index, 2), 0, kv_count * half :].astype(F32)
            return digits[2 * phase : 2 * phase + 1, 0:1] * 64.0 + digits[
                2 * phase + 1 : 2 * phase + 2, 0:1
            ]

        key_pos = jnp.zeros(lanes.shape, F32)
        for index, source in enumerate(sources):
            within = (lanes >= index * half) & (lanes < (index + 1) * half)
            key_pos = jnp.where(within, base(source) + (lanes - index * half).astype(F32), key_pos)
        return jnp.where(key_pos <= base(me) + rows, 0.0, MASKED)

    stack = group if keys <= 1024 else 1
    heads = range(0, kv_count * group, stack)
    slope = LOG2E / math.sqrt(HEAD)

    def queries_of(phase, head):
        return jnp.concatenate(
            [query[phase, :, (head + i) * HEAD : (head + i + 1) * HEAD] for i in range(stack)],
            axis=0,
        )

    def scores_of(block_rows, key_rows, mask):
        count = key_rows.shape[0]
        value = lax.dot_general(
            block_rows, key_rows, (((1,), (1,)), ((), ())), preferred_element_type=F32
        ).reshape(stack, half, count)
        return value if mask is None else value + mask[None]

    def weigh(value, peak):
        weights = jnp.exp2((value - peak) * slope)
        return jnp.sum(weights, axis=2, keepdims=True), weights.astype(BF16)

    def mix(weights, value_rows):
        return jnp.dot(
            weights.reshape(stack * half, weights.shape[2]), value_rows,
            preferred_element_type=F32,
        ).reshape(stack, half, HEAD)

    def head_rows(phase, place, kind, kv_head):
        span_of = slice(kv_head * half, (kv_head + 1) * half)
        if place is None:
            return kv[phase, :, :, kind, span_of].reshape(keys, HEAD)
        return kv[phase, :, place, kind, span_of].reshape(line * half, HEAD)

    def put(phase, head, mixed):
        for i in range(stack):
            attended[phase, :, (head + i) * HEAD : (head + i + 1) * HEAD] = mixed[i].astype(BF16)

    def column_scores(place):
        mask = bias(0, [2 * index + place for index in range(line)])
        values = []
        for head in heads:
            value = scores_of(
                queries_of(0, head), head_rows(0, place, 0, head // group), mask
            )
            values.append((value, jnp.max(value, axis=2, keepdims=True)))
        return values

    def attend_near():
        results = []
        for head, (value, peak) in zip(heads, column_scores(column)):
            total, weights = weigh(value, peak)
            results.append((peak, total, mix(weights, head_rows(0, column, 1, head // group))))
        return results

    def weigh_far(near):
        results = []
        for (old_peak, old_total, _), (value, peak) in zip(near, column_scores(1 - column)):
            peak = jnp.maximum(peak, old_peak)
            total, weights = weigh(value, peak)
            shrink = jnp.exp2((old_peak - peak) * slope)
            inverse = 1.0 / (total + old_total * shrink)
            results.append((weights, inverse, shrink * inverse))
        return results

    def attend_far(near, far):
        for head, (_, _, old_mixed), (weights, inverse, shrink) in zip(heads, near, far):
            mixed = mix(weights, head_rows(0, 1 - column, 1, head // group))
            put(0, head, mixed * inverse + old_mixed * shrink)

    def attend(phase):
        mask = bias(phase, list(range(n_seq)))
        for head in heads:
            kv_head = head // group
            block_rows = queries_of(phase, head)
            scores = [
                scores_of(
                    block_rows, head_rows(piece, None, 0, kv_head),
                    mask if piece == phase else None,
                )
                for piece in range(phase + 1)
            ]
            peak = jnp.max(scores[0], axis=2, keepdims=True)
            for value in scores[1:]:
                peak = jnp.maximum(peak, jnp.max(value, axis=2, keepdims=True))
            mixed = jnp.zeros((stack, half, HEAD), F32)
            total = jnp.zeros((stack, half, 1), F32)
            for piece, value in enumerate(scores):
                more, weights = weigh(value, peak)
                total += more
                mixed += mix(weights, head_rows(piece, None, 1, kv_head))
            put(phase, head, mixed / total)

    starts = group_starts(len(tiles))

    def slot_of(phase, index):
        return 0 if phase == 0 else sum(1 for start in starts if start <= index)

    def reduce_tile(phase, index):
        columns = tiles[index][2]
        landed(from_core.at[phase, :, columns], core_recv.at[phase, index])
        both = part[phase, core, :, columns].astype(F32) + from_core[phase, :, columns].astype(F32)
        pair[phase, y, :, columns] = both.astype(BF16)
        for step in range(1, n_y):
            target = lax.rem(y + step, n_y) * 2 + core
            remote(
                pair.at[phase, y, :, columns], pair.at[phase, y, :, columns],
                y_send.at[phase, step - 1], y_recv.at[n_y - 1 - step, slot_of(phase, index)], (me, target),
            )

    def project(phase, between):
        done = 0
        for index, (part_of, inner, columns) in enumerate(tiles):
            product = jnp.dot(
                attended[phase], weight[:, columns], preferred_element_type=F32
            )
            mine = jnp.where(tp == part_of, 1.0, 0.0)
            product += residual[phase, :, inner].astype(F32) * mine
            part[phase, 0, :, columns] = product[:own].astype(BF16)
            part[phase, 1, :, columns] = product[own:].astype(BF16)
            remote(
                part.at[phase, 1 - core, :, columns], from_core.at[phase, :, columns],
                core_send.at[phase], core_recv.at[phase, index], (me, core_peer),
            )
            ready = 1 if index < 4 else 2
            while done + ready <= index:
                reduce_tile(phase, done)
                done += 1
            for place, task in between:
                if min(place, len(tiles) - 1) == index:
                    task()
        for index in range(done, len(tiles)):
            reduce_tile(phase, index)

    def finish(phase):
        square = jnp.zeros((own, 1), F32)
        peak = jnp.zeros((own, 1), F32)
        for index, (part_of, inner, columns) in enumerate(tiles):
            groups = starts if phase else [0]
            if index in groups:
                end = min([start for start in groups if start > index] + [len(tiles)]) - 1
                wanted = slice(columns.start, tiles[end][2].stop)
                for step in range(1, n_y):
                    source = lax.rem(y + step, n_y)
                    landed(
                        pair.at[phase, source, :, wanted],
                        y_recv.at[step - 1, slot_of(phase, index)],
                    )
            total = pair[phase, 0, :, columns].astype(F32)
            for source in range(1, n_y):
                total += pair[phase, source, :, columns].astype(F32)
            total_all[phase, part_of, core, :, inner] = total.astype(BF16)
            piece = total_all.at[phase, part_of, core, :, inner]
            remote(piece, piece, out_send.at[phase], out_recv.at[phase], (me, core_peer))
            square += jnp.sum(total * total, axis=1, keepdims=True)
            scaled = total * gain_all[part_of, :, inner]
            peak = jnp.maximum(peak, jnp.max(jnp.abs(scaled), axis=1, keepdims=True))
        inverse = lax.rsqrt(square / model + 1e-5)
        token = inverse * peak + 1e-6
        stat[phase, core, 0] = jnp.broadcast_to(token, (own, 128))
        stat[phase, core, 1] = jnp.broadcast_to(inverse / token, (own, 128))
        remote(
            stat.at[phase, core], stat.at[phase, core], stat_send.at[phase],
            stat_recv.at[phase], (me, core_peer),
        )

    def sends_left(phase):
        for step in range(1, n_y):
            left(pair.at[phase, y], y_send.at[phase, step - 1])
        left(total_all.at[phase, :, core], out_send.at[phase])
        left(stat.at[phase, core], stat_send.at[phase])

    def totals_landed(phase):
        landed(total_all.at[phase, :, 1 - core], out_recv.at[phase])
        landed(stat.at[phase, 1 - core], stat_recv.at[phase])

    def normalize(phase, owner, slot):
        factor = stat[phase, owner, 1][:, 0:1]
        for part_of in range(n_tp):
            value = total_all[phase, part_of, owner].astype(F32) * gain_all[part_of]
            columns = slice(part_of * slice_width, (part_of + 1) * slice_width)
            ready[slot, :, columns] = (value * factor).astype(BF16)

    near = attend_near()
    arrivals(0)
    far = weigh_far(near)
    arrivals(1)
    attend_far(near, far)
    loads[6].wait()
    later = [d for d in (1, 3, 2) if d < line] + list(range(4, line))
    project(
        0,
        [
            (1 + 2 * i, functools.partial(relay, (2,), side, distance))
            for i, distance in enumerate(later)
            for side in (-1, 1)
        ],
    )
    arrivals(2)
    attend(1)
    project(1, [])
    landed(gain_all.at[0 : n_tp - 1], gain_recv.at[0])
    finish(0)
    totals_landed(0)
    for owner in range(2):
        normalize(0, owner, owner)
    sends_left(0)
    left_all()
    for phase in range(2):
        left(part.at[phase, 1 - core], core_send.at[phase])
    left(gain_all.at[0 : n_tp - 1], gain_send.at[0])
    finish(1)
    normalize(1, core, 2)
    totals_landed(1)
    sends_left(1)


def assemble(
    dims, total_all, ready, stat, gain_all, order_ref, quant_hbm, scale_hbm, stream_hbm,
    quant, scale_row, sem,
):
    n_tp, own, slice_width = dims
    tp = lax.axis_index("tp")
    swap = (order_ref[0, 0] < 0.5).astype(jnp.int32)
    mine = lax.rem(tp, 2)

    def send(src, dst, index):
        pltpu.make_async_copy(src, dst, sem.at[index]).start()

    def rows(phase, core, first=0, count=own):
        place = swap if phase == 0 else 1 - swap
        start = pl.multiple_of((2 * place + core) * own, own) + first
        return pl.ds(pl.multiple_of(start, count), count)

    def send_rows(slot, phase, core):
        count = math.gcd(own, 16)
        for first in range(0, own, count):
            send(
                ready.at[slot, first : first + count],
                quant_hbm.at[rows(phase, core, first, count)], 0,
            )

    for core in range(2):
        send_rows(core, 0, core)
    send_rows(2, 1, mine)
    for core in range(2):
        for phase in range(2):
            send(total_all.at[phase, tp, core], stream_hbm.at[rows(phase, core)], 1)
    factor = stat[1, 1 - mine, 1][:, 0:1]
    for part in range(n_tp):
        columns = slice(part * slice_width, (part + 1) * slice_width)
        value = total_all[1, part, 1 - mine].astype(F32) * gain_all[part]
        quant[:, columns] = (value * factor).astype(BF16)
        send(quant.at[:, columns], quant_hbm.at[rows(1, 1 - mine), columns], 0)
    scale = jnp.concatenate(
        [stat[swap if top == 0 else 1 - swap, core, 0] for top in range(2) for core in range(2)],
        axis=0,
    )
    count = 4 * own
    row = lax.broadcasted_iota(jnp.int32, (count, 128), 0)
    lane = lax.broadcasted_iota(jnp.int32, (count, 128), 1)
    for start in range(0, count, 128):
        piece = jnp.sum(jnp.where(row == lane + start, scale, 0.0), axis=0, keepdims=True)
        width = min(128, count - start)
        scale_row[:, start : start + width] = piece[:, :width]
    send(scale_row, scale_hbm, 2)
    for index, array in enumerate((quant_hbm, stream_hbm, scale_hbm)):
        pltpu.make_async_copy(array, array, sem.at[index]).wait()


def group_starts(count):
    if count < 6:
        return list(range(count))
    return [0] + list(range(4, count - 2, 2)) + [count - 2, count - 1]


def tiles_of(n_tp, slice_width):
    if slice_width % 768:
        widths = [[slice_width]] * n_tp
    else:
        first = [256, 512] + [768] * (slice_width // 768 - 1)
        widths = [first] + [[768] * (slice_width // 768)] * (n_tp - 2) + [first[::-1]]
    tiles = []
    for index, row in enumerate(widths):
        inner = 0
        for width in row:
            start = index * slice_width + inner
            tiles.append((index, slice(inner, inner + width), slice(start, start + width)))
            inner += width
    return tiles


def on_device(n_seq, n_tp, queries, key_vectors, value_vectors, positions, residual, norm_gain, out_weight):
    token_rows, query_width = queries.shape
    half = token_rows // 2
    own = half // 2
    kv_width = key_vectors.shape[1]
    kv_count = kv_width // HEAD
    group = query_width // kv_width
    model = out_weight.shape[1]
    slice_width = residual.shape[1]
    tiles = tiles_of(n_tp, slice_width)
    count = len(tiles)
    n_y = n_tp // 2
    vmem = pl.BlockSpec(memory_space=pltpu.VMEM)
    anywhere = pl.BlockSpec(memory_space=pl.ANY)
    dma = pltpu.SemaphoreType.DMA
    line = n_seq // 2
    middle = pl.pallas_call(
        functools.partial(kernel, (n_seq, n_tp, group, kv_count, half, tiles)),
        out_shape=(
            pltpu.VMEM((2, n_tp, 2, own, slice_width), BF16),
            pltpu.VMEM((3, own, model), BF16),
            pltpu.VMEM((2, 2, 2, own, 128), F32),
            pltpu.VMEM((n_tp, 1, slice_width), F32),
            pltpu.VMEM((8, 128), F32),
        ),
        in_specs=[anywhere] * 7,
        out_specs=(vmem,) * 5,
        scratch_shapes=[
            pltpu.VMEM((2, line, 2, 2, kv_count * half + 16, HEAD), BF16),
            pltpu.VMEM((1, token_rows), jnp.int32),
            pltpu.VMEM(key_vectors.shape, BF16),
            pltpu.VMEM(value_vectors.shape, BF16),
            pltpu.VMEM(queries.shape, BF16),
            pltpu.VMEM(residual.shape, BF16),
            pltpu.VMEM((2, half, query_width), BF16),
            pltpu.VMEM((2, half, slice_width), BF16),
            pltpu.VMEM(out_weight.shape, BF16),
            pltpu.VMEM((2, half, query_width), BF16),
            pltpu.VMEM((2, 2, own, model), BF16),
            pltpu.VMEM((2, own, model), BF16),
            pltpu.VMEM((2, n_y, own, model), BF16),
            dma((7,)),
            dma((3,)),
            dma((3,)),
            dma((3, 2)),
            dma((3, line)),
            dma((1,)),
            dma((1,)),
            dma((2,)),
            dma((2, count)),
            dma((2, n_y - 1)),
            dma((n_y - 1, 1 + len(group_starts(count)))),
            dma((2,)),
            dma((2,)),
            dma((2,)),
            dma((2,)),
        ],
        compiler_params=pltpu.CompilerParams(
            collective_id=0, has_side_effects=True, vmem_limit_bytes=48 * 1024 * 1024
        ),
    )(
        *(
            pltpu.with_memory_space_constraint(value, pltpu.HBM)
            for value in (
                positions[None, :], key_vectors, value_vectors, norm_gain, queries, residual,
                out_weight,
            )
        )
    )
    quant, scale, stream = pl.pallas_call(
        functools.partial(assemble, (n_tp, own, slice_width)),
        out_shape=(
            jax.ShapeDtypeStruct((token_rows, model), BF16),
            jax.ShapeDtypeStruct((1, token_rows), F32),
            jax.ShapeDtypeStruct((token_rows, slice_width), BF16),
        ),
        in_specs=[vmem] * 5,
        out_specs=(anywhere,) * 3,
        scratch_shapes=[
            pltpu.VMEM((own, model), BF16),
            pltpu.VMEM((1, token_rows), F32),
            dma((3,)),
        ],
        compiler_params=pltpu.CompilerParams(vmem_limit_bytes=12 * 1024 * 1024),
    )(*middle)
    return (quant, scale.reshape(token_rows), stream)


def solution(mesh):
    return jax.shard_map(
        functools.partial(on_device, mesh.shape["seq"], mesh.shape["tp"]),
        mesh=mesh,
        in_specs=(
            P("seq", "tp"),
            P("seq", "tp"),
            P("seq", "tp"),
            P("seq"),
            P("seq", "tp"),
            P(None, "tp"),
            P("tp", None),
        ),
        out_specs=(P("seq", None), P("seq"), P("seq", "tp")),
        check_vma=False,
    )
```
